512 devices in a mesh: job: 2 (over y), row: 16 (over z), col: 8 (over x), samp: 2 (over core).
Axes of the slice: x: 8, y: 2, z: 16, core: 2. Of those that a mesh axis runs over, the one named last changes fastest.
The devices are a block of a 8x8x16 slice.
Arguments:
- pair_repr: bfloat16 [1024, 512, 128], P(('job', 'row'), ('col', 'samp')), parts along dimension 0, may hold values from -100 to 100
- asym_id: int32 [1024], P('job'), parts along dimension 0, may hold values from 0 to 7, never falling along the last dimension, each value on 1 to 128 neighbouring positions
- valid_len: int32 [2], P('job'), parts along dimension 0, may hold values from 256 to 512
- rel_embed: bfloat16 [128, 128], replicated, may hold values from -12 to 12
- pair_gain: float32 [128], replicated, may hold values from 0.25 to 1.75
- bias_weight: bfloat16 [128, 16], replicated, may hold values from -64 to 64
- tokens: bfloat16 [128, 512, 768], P(('job', 'col', 'samp'), 'row'), parts along dimension 0, may hold values from -6 to 6
- token_gain: float32 [1, 768], replicated, may hold values from 0.25 to 1.75
- qkv_weight: bfloat16 [1, 3, 768, 768], P(None, None, None, 'row'), may hold values from -0.21875 to 0.21875
- out_weight: bfloat16 [1, 768, 768], P(None, 'row'), may hold values from -0.21875 to 0.21875
Outputs:
- refined: bfloat16 [128, 512, 768], P(('job', 'col', 'samp'), 'row'), parts along dimension 0
The draws below stay inside these ranges and needn't reach their ends.
There are 2 independent parts, one for each index of `job`. The reference program is written for one: setup_inputs(seed, part) draws one part's arguments, and reference() takes and returns one part's arrays. A program takes and returns all parts, laid end to end along the dimension named above; an argument that names none is the same for every part. Nothing has to cross between parts.
Inputs may be any that keep to these rules, and one draw needn't show every extreme that they name: `asym_id`: chain indices never fall along the tokens.
All inputs are finite; a program needn't handle non-finite values.
Results may differ from the reference program's by a relative error of at most 0.002.
The reference program's roundings to bfloat16 on the way count: a program that leaves them out, or rounds other values in their place, can miss the bound.
Values may be sent and summed in bfloat16 or wider, within the bound.
No kernel may reach another device: no remote copies, remote signals or barrier semaphores. Data moves between devices by JAX's collectives and lax.ppermute only.
A program may use at most 64 MiB of HBM per device.

```python
import math
import jax
import jax.numpy as jnp
import numpy as np
from jax import lax

PAIR_C = 128
D = 768
HEADS = 16
HEAD_DIM = 48
REL = 128
LAYERS = 1
TOKENS = 512
SAMPLES = 64
N_ROW = 16


def draw_pair_repr(key, part):
    noise_key, scale_key = jax.random.split(key, 2)
    scales = jnp.exp(jax.random.uniform(scale_key, (TOKENS, TOKENS, 1), jnp.float32, 0.0, math.log(10.0)))
    values = jax.random.normal(noise_key, (TOKENS, TOKENS, PAIR_C), jnp.float32) * scales
    return jnp.clip(values, -100.0, 100.0).astype(jnp.bfloat16)


def draw_bias_weight(key, part):
    noise_key = jax.random.fold_in(key, 0)
    strength = jnp.full((1, HEADS), 2.5, jnp.float32)
    spread = strength / math.sqrt(PAIR_C)
    values = jax.random.normal(noise_key, (PAIR_C, HEADS), jnp.float32) * spread
    return jnp.clip(values, -6.0 * spread, 6.0 * spread).astype(jnp.bfloat16)


def level_of(key, dims, cuts, smallest, top_value):
    factor_of, own = 1.0, jax.random.fold_in(key, 6)
    for position, shards_of in cuts:
        draws = jnp.exp(jax.random.uniform(jax.random.fold_in(own, position), (shards_of,), jnp.float32, smallest / len(cuts), top_value / len(cuts)))
        factor_of = factor_of * jnp.repeat(draws, dims[position] // shards_of).reshape([-1 if axis == position else 1 for axis in range(len(dims))])
    return factor_of


def length_profile(amount, total, most, skew):
    weights = [(1 << 20) // math.isqrt(rank ** skew) + 1 for rank in range(2, amount + 1)]
    spare, holding = total - most - (amount - 1), [1] * (amount - 1)
    while spare > 0:
        movable = [i for i in range(amount - 1) if holding[i] < most]
        pool, budget = sum([weights[i] for i in movable]), spare
        for i in movable:
            addition = min(most - holding[i], max(1, budget * weights[i] // pool), spare)
            holding[i] = holding[i] + addition
            spare = spare - addition
    return np.array([most] + holding)


def uneven(own_key, count, total, limit, skew):
    if count == 2:
        one = jax.random.randint(own_key, (), max(1, total - limit), min(limit, total - 1) + 1)
        return jnp.stack([one, total - one])
    sizes = jnp.asarray(length_profile(count, total, limit, skew), jnp.int32)
    couples = (count - 1) // 2
    giver, sink = sizes[1:1 + 2 * couples:2], sizes[2:2 + 2 * couples:2]
    room = jnp.minimum(giver - 1, limit - sink)
    moved = jax.random.randint(jax.random.fold_in(own_key, 1), (couples,), 0, 1 << 20) % (room + 1)
    sizes = sizes.at[1:1 + 2 * couples:2].set(giver - moved).at[2:2 + 2 * couples:2].set(sink + moved)
    return sizes[jax.random.permutation(jax.random.fold_in(own_key, 2), count)]


def normal_values(stream_key, shape, deviation, reach, shards=(), held_as=jnp.bfloat16):
    array = jax.random.normal(stream_key, shape, jnp.float32) * deviation
    if len(shards) > 0:
        array = level_of(stream_key, shape, shards, -0.22, 0.18) * array
    return jnp.clip(array, min=-reach, max=reach).astype(held_as)


def setup_inputs(seed: int = 0, part: int = 0) -> dict:
    arg_keys = jax.random.split(jax.random.key(seed), 11)
    own_keys = jax.random.split(jax.random.fold_in(arg_keys[10], part), 11)
    pair_repr = draw_pair_repr(jax.random.fold_in(jax.random.fold_in(arg_keys[10], part), 71), part)
    asym_id = jnp.searchsorted(jnp.cumsum(uneven(own_keys[1], 8, TOKENS, TOKENS // 4, 1)), jnp.arange(TOKENS), side="right").astype(jnp.int32)
    valid_len = jax.random.randint(own_keys[2], (1,), TOKENS // 2, TOKENS + 1).astype(jnp.int32)
    rel_embed = normal_values(arg_keys[3], (REL, PAIR_C), 2.0, 12.0)
    pair_gain = jnp.clip(1.0 + 0.15 * jax.random.normal(arg_keys[4], (PAIR_C,), jnp.float32), 0.25, 1.75)
    bias_weight = draw_bias_weight(jax.random.fold_in(arg_keys[10], 71), part)
    tokens = normal_values(own_keys[6], (SAMPLES, TOKENS, D), 1.0, 6.0, ((0, 16), (1, 16)))
    token_gain = jnp.clip(1.0 + 0.15 * jax.random.normal(arg_keys[7], (LAYERS, D), jnp.float32), 0.25, 1.75)
    qkv_weight = normal_values(arg_keys[8], (LAYERS, 3, D, D), D ** -0.5, 0.21875, ((3, 16),))
    out_weight = normal_values(arg_keys[9], (LAYERS, D, D), D ** -0.5, 0.21875, ((1, 16),))
    return dict(pair_repr=pair_repr, asym_id=asym_id, valid_len=valid_len, rel_embed=rel_embed, pair_gain=pair_gain, bias_weight=bias_weight, tokens=tokens, token_gain=token_gain, qkv_weight=qkv_weight, out_weight=out_weight)


epsilon = 1e-05

def normalize(values, gain_vector):
    average = lax.optimization_barrier(jnp.mean(values, axis=-1, keepdims=True))
    centered = values - average
    variance = lax.optimization_barrier(jnp.mean(centered * centered, axis=-1, keepdims=True))
    return centered * lax.rsqrt(variance + epsilon) * gain_vector

def attend_sample(queries, key_rows, value_rows, pair_bias, keymask):
    query_f = queries.astype(jnp.float32).reshape(TOKENS, HEADS, HEAD_DIM)
    key_f = key_rows.astype(jnp.float32).reshape(TOKENS, HEADS, HEAD_DIM)
    value_f = value_rows.astype(jnp.float32).reshape(TOKENS, HEADS, HEAD_DIM)
    scores = jnp.einsum('ihd,jhd->hij', query_f, key_f) / math.sqrt(HEAD_DIM) + pair_bias
    scores = jnp.where(keymask[None, None, :], scores, -1e+30)
    row_max = lax.optimization_barrier(jnp.max(scores, axis=-1, keepdims=True))
    weights = jnp.where(keymask[None, None, :], jnp.exp(scores - row_max), 0.0)
    row_total = lax.optimization_barrier(jnp.sum(weights, axis=-1, keepdims=True))
    probs = (weights / row_total).astype(jnp.bfloat16)
    attended = jnp.einsum('hij,jhd->ihd', probs.astype(jnp.float32), value_f)
    return attended.reshape(TOKENS, D).astype(jnp.bfloat16)

def reference(pair_repr, asym_id, valid_len, rel_embed, pair_gain, bias_weight, tokens, token_gain, qkv_weight, out_weight):
    block_rows = TOKENS // N_ROW
    positions = jnp.arange(TOKENS, dtype=jnp.int32)
    reach_max = REL // 2 - 1

    def bias_block(block_index):
        first_row = (block_index * block_rows).astype(jnp.int32)
        pair_rows = lax.dynamic_slice_in_dim(pair_repr, first_row, block_rows, 0)
        row_ids = first_row + jnp.arange(block_rows, dtype=jnp.int32)
        row_chain = lax.dynamic_slice_in_dim(asym_id, first_row, block_rows, 0)
        offset = jnp.clip(row_ids[:, None] - positions[None, :], -reach_max, reach_max) + reach_max
        bin_ids = jnp.where(row_chain[:, None] == asym_id[None, :], offset, REL - 1)
        onehot = (bin_ids.reshape(-1)[:, None] == jnp.arange(REL, dtype=jnp.int32)[None, :]).astype(jnp.bfloat16)
        summed = pair_rows.reshape(-1, PAIR_C).astype(jnp.float32) + jnp.dot(onehot, rel_embed, preferred_element_type=jnp.float32)
        normed = normalize(summed, pair_gain).astype(jnp.bfloat16)
        projected = lax.dot_general(bias_weight, normed, (((0,), (1,)), ((), ())), preferred_element_type=jnp.float32)
        return projected.reshape(HEADS, block_rows, TOKENS)
    blocks = lax.map(bias_block, jnp.arange(N_ROW, dtype=jnp.int32))
    pair_bias = jnp.transpose(blocks, (1, 0, 2, 3)).reshape(HEADS, TOKENS, TOKENS)
    keymask = positions < valid_len[0]
    current = tokens
    for layer_index in range(LAYERS):
        normed_tok = normalize(current.astype(jnp.float32), token_gain[layer_index]).astype(jnp.bfloat16)
        flat = normed_tok.reshape(-1, D)
        parts = []
        for part_index in range(3):
            product = jnp.dot(flat, qkv_weight[layer_index, part_index], preferred_element_type=jnp.float32)
            parts.append(product.astype(jnp.bfloat16).reshape(SAMPLES, TOKENS, D))

        def one_sample(sample_item):
            return attend_sample(sample_item[0], sample_item[1], sample_item[2], pair_bias, keymask)
        attended = lax.map(one_sample, (parts[0], parts[1], parts[2]))
        update = jnp.dot(attended.reshape(-1, D), out_weight[layer_index], preferred_element_type=jnp.float32)
        current = (current.astype(jnp.float32) + update.reshape(SAMPLES, TOKENS, D)).astype(jnp.bfloat16)
    return current
```

```python
import math

import jax
import jax.numpy as jnp
from jax import lax
from jax.sharding import PartitionSpec as P

HEAD_DIM = 48
QUAD = 4

epsilon = 1e-05


def normalize(values, gain_vector):
    average = jnp.mean(values, axis=-1, keepdims=True)
    centered = values - average
    variance = jnp.mean(centered * centered, axis=-1, keepdims=True)
    return centered * lax.rsqrt(variance + epsilon) * gain_vector


def exchange(blocks, axis, groups=None):
    return lax.all_to_all(
        blocks, axis, split_axis=0, concat_axis=0, axis_index_groups=groups, tiled=True
    )


def bias_tile_of(pair_repr, asym_id, rel_embed, pair_gain, bias_weight):
    tile_rows, tile_cols, channels = pair_repr.shape
    bin_count = rel_embed.shape[0]
    reach_max = bin_count // 2 - 1
    first_row = lax.axis_index("row") * tile_rows
    first_col = lax.axis_index(("col", "samp")) * tile_cols
    row_ids = first_row + jnp.arange(tile_rows, dtype=jnp.int32)
    col_ids = first_col + jnp.arange(tile_cols, dtype=jnp.int32)
    row_chain = lax.dynamic_slice_in_dim(asym_id, first_row, tile_rows, 0)
    col_chain = lax.dynamic_slice_in_dim(asym_id, first_col, tile_cols, 0)
    offset = jnp.clip(row_ids[:, None] - col_ids[None, :], -reach_max, reach_max) + reach_max
    bin_ids = jnp.where(row_chain[:, None] == col_chain[None, :], offset, bin_count - 1)
    onehot = (
        bin_ids.reshape(-1)[:, None] == jnp.arange(bin_count, dtype=jnp.int32)[None, :]
    ).astype(jnp.bfloat16)
    summed = pair_repr.reshape(-1, channels).astype(jnp.float32) + jnp.dot(
        onehot, rel_embed, preferred_element_type=jnp.float32
    )
    normed = normalize(summed, pair_gain).astype(jnp.bfloat16)
    projected = lax.dot_general(
        bias_weight, normed, (((0,), (1,)), ((), ())), preferred_element_type=jnp.float32
    )
    return projected


def per_device(
    pair_repr,
    asym_id,
    valid_len,
    rel_embed,
    pair_gain,
    bias_weight,
    tokens,
    token_gain,
    qkv_weight,
    out_weight,
):
    sample_count, token_rows, width = tokens.shape
    total = asym_id.shape[0]
    rows = lax.axis_size("row")
    cols = lax.axis_size("col")
    tile_rows, tile_cols, _ = pair_repr.shape
    heads = bias_weight.shape[1]
    quads = rows // QUAD
    strided = [[a + QUAD * b for b in range(quads)] for a in range(QUAD)]
    adjacent = [[QUAD * a + b for b in range(QUAD)] for a in range(quads)]
    z = lax.axis_index("row")
    side = (z // QUAD) % 2
    core = lax.axis_index("samp")
    swap = [(0, 1), (1, 0)]
    keymask = jnp.arange(total, dtype=jnp.int32) < valid_len[0]
    score_scale = 1.0 / math.sqrt(HEAD_DIM)

    own_w = qkv_weight[0]
    half = width // 2
    part = lax.dynamic_slice_in_dim(own_w, core * half, half, 1)
    far = lax.ppermute(part, "row", [(i, i ^ QUAD) for i in range(rows)])
    near = lax.ppermute(far, "samp", swap)
    other_w = jnp.where(
        core == 0, jnp.concatenate([far, near], 1), jnp.concatenate([near, far], 1)
    )
    own_first = side == core
    w_a = jnp.where(own_first, own_w, other_w)
    w_b = jnp.where(own_first, other_w, own_w)
    w_pair = jnp.stack([w_a, w_b])

    paired = bias_weight.reshape(-1, heads // 8, 2, QUAD).transpose(0, 1, 3, 2).reshape(-1, heads)
    tile = bias_tile_of(pair_repr, asym_id, rel_embed, pair_gain, paired)
    tile = tile.reshape(heads // 8, 1, QUAD, 2, tile_rows * tile_cols)
    tile = jnp.broadcast_to(tile, (heads // 8, 2, QUAD, 2, tile_rows * tile_cols))
    by_row = exchange(tile.reshape(rows, 2, tile_rows * tile_cols), "row")
    by_key = by_row.reshape(rows, 2, tile_rows, tile_cols).transpose(1, 3, 0, 2)
    by_key = by_key.reshape(1, 2, tile_cols, total)
    fanned = jnp.broadcast_to(by_key, (cols, 2, tile_cols, total)).reshape(
        2 * cols, tile_cols, total
    )
    bias_a = exchange(fanned, ("col", "samp")).reshape(total, total)
    bias_b = lax.ppermute(bias_a, "samp", swap)
    biases = jnp.stack([bias_a, bias_b])

    normed = normalize(tokens.astype(jnp.float32), token_gain[0]).astype(jnp.bfloat16)
    halves = normed.reshape(2, sample_count // 2 * token_rows, width)
    gathered = exchange(jnp.concatenate([halves] * (quads // 2)), "row", strided)
    gathered = jnp.broadcast_to(gathered[None], (QUAD, *gathered.shape))
    gathered = exchange(gathered, "row", adjacent)
    gathered = gathered.reshape(QUAD, quads, sample_count // 2, token_rows, width)
    gathered = gathered.transpose(2, 1, 0, 3, 4).reshape(sample_count // 2, total, width)

    depth = out_weight.shape[1]
    slice_rows = depth // cols
    piece = lax.dynamic_slice_in_dim(
        out_weight[0], lax.axis_index("col") * slice_rows, slice_rows, 0
    )
    pieces = exchange(jnp.broadcast_to(piece[None], (rows, *piece.shape)), "row")
    pieces = exchange(
        jnp.broadcast_to(pieces.reshape(1, rows * slice_rows, width), (cols, rows * slice_rows, width)),
        "col",
    )
    w_out = pieces.reshape(cols, rows // 8, 2, QUAD, slice_rows, width)
    w_out = w_out.transpose(1, 3, 2, 0, 4, 5).reshape(width, width)

    projected = jnp.einsum(
        "snc,hpcw->pshnw", gathered, w_pair, preferred_element_type=jnp.float32
    ).astype(jnp.bfloat16)
    query, key, value = projected[0], projected[1], projected[2]
    scores = (
        jnp.einsum("shjd,shid->shji", key, query, preferred_element_type=jnp.float32) * score_scale
        + biases[None]
    )
    mask = keymask[None, None, :, None]
    scores = jnp.where(mask, scores, -1e30)
    row_max = jnp.max(scores, axis=2, keepdims=True)
    weights = jnp.where(mask, jnp.exp(scores - row_max), 0.0)
    row_total = jnp.sum(weights, axis=2, keepdims=True)
    probs = (weights / row_total).astype(jnp.bfloat16)
    attended = jnp.einsum(
        "shji,shjd->sihd", probs, value, preferred_element_type=jnp.float32
    ).astype(jnp.bfloat16)
    attended = jnp.where(core == 0, attended, attended[:, :, ::-1])

    back = attended.reshape(sample_count // 2, rows, token_rows, 2 * HEAD_DIM)
    back = exchange(back.transpose(1, 0, 2, 3), "row")
    back = back.reshape(rows // 8, 2, QUAD, sample_count // 2, token_rows, 2 * HEAD_DIM)
    back = back.transpose(1, 3, 4, 0, 2, 5).reshape(sample_count * token_rows, width)
    update = jnp.dot(back, w_out, preferred_element_type=jnp.float32)
    return (
        tokens.astype(jnp.float32) + update.reshape(sample_count, token_rows, width)
    ).astype(jnp.bfloat16)


def solution(mesh):
    return jax.shard_map(
        per_device,
        mesh=mesh,
        in_specs=(
            P(("job", "row"), ("col", "samp"), None),
            P("job"),
            P("job"),
            P(),
            P(),
            P(),
            P(("job", "col", "samp"), "row", None),
            P(),
            P(None, None, None, "row"),
            P(None, "row", None),
        ),
        out_specs=P(("job", "col", "samp"), "row", None),
        check_vma=False,
    )
```

```python
import math

import jax
import jax.numpy as jnp
from jax import lax
from jax.sharding import PartitionSpec as P

HEAD_DIM = 48
QUAD = 4

epsilon = 1e-05


def normalize(values, gain_vector):
    average = jnp.mean(values, axis=-1, keepdims=True)
    centered = values - average
    variance = jnp.mean(centered * centered, axis=-1, keepdims=True)
    return centered * lax.rsqrt(variance + epsilon) * gain_vector


def exchange(blocks, axis, groups=None):
    return lax.all_to_all(
        blocks, axis, split_axis=0, concat_axis=0, axis_index_groups=groups, tiled=True
    )


def bias_tile_of(pair_repr, asym_id, rel_embed, pair_gain, bias_weight):
    tile_rows, tile_cols, channels = pair_repr.shape
    bin_count = rel_embed.shape[0]
    reach_max = bin_count // 2 - 1
    first_row = lax.axis_index("row") * tile_rows
    first_col = lax.axis_index(("col", "samp")) * tile_cols
    row_ids = first_row + jnp.arange(tile_rows, dtype=jnp.int32)
    col_ids = first_col + jnp.arange(tile_cols, dtype=jnp.int32)
    row_chain = lax.dynamic_slice_in_dim(asym_id, first_row, tile_rows, 0)
    col_chain = lax.dynamic_slice_in_dim(asym_id, first_col, tile_cols, 0)
    offset = jnp.clip(row_ids[:, None] - col_ids[None, :], -reach_max, reach_max) + reach_max
    bin_ids = jnp.where(row_chain[:, None] == col_chain[None, :], offset, bin_count - 1)
    onehot = (
        bin_ids.reshape(-1)[:, None] == jnp.arange(bin_count, dtype=jnp.int32)[None, :]
    ).astype(jnp.bfloat16)
    summed = pair_repr.reshape(-1, channels).astype(jnp.float32) + jnp.dot(
        onehot, rel_embed, preferred_element_type=jnp.float32
    )
    normed = normalize(summed, pair_gain).astype(jnp.bfloat16)
    projected = lax.dot_general(
        bias_weight, normed, (((0,), (1,)), ((), ())), preferred_element_type=jnp.float32
    )
    return projected


def per_device(
    pair_repr,
    asym_id,
    valid_len,
    rel_embed,
    pair_gain,
    bias_weight,
    tokens,
    token_gain,
    qkv_weight,
    out_weight,
):
    sample_count, token_rows, width = tokens.shape
    total = asym_id.shape[0]
    rows = lax.axis_size("row")
    cols = lax.axis_size("col")
    tile_rows, tile_cols, _ = pair_repr.shape
    heads = bias_weight.shape[1]
    quads = rows // QUAD
    adjacent = [[QUAD * a + b for b in range(QUAD)] for a in range(quads)]
    z = lax.axis_index("row")
    side = (z // QUAD) % 2
    core = lax.axis_index("samp")
    swap = [(0, 1), (1, 0)]
    keymask = jnp.arange(total, dtype=jnp.int32) < valid_len[0]
    score_scale = 1.0 / math.sqrt(HEAD_DIM)

    def shifted(value, axis, by):
        size = lax.axis_size(axis)
        return lax.ppermute(value, axis, [(i, (i + by) % size) for i in range(size)])

    own_w = qkv_weight[0]
    half = width // 2
    part = lax.dynamic_slice_in_dim(own_w, core * half, half, 1)
    far = lax.ppermute(part, "row", [(i, i ^ QUAD) for i in range(rows)])
    near = lax.ppermute(far, "samp", swap)
    other_w = jnp.where(
        core == 0, jnp.concatenate([far, near], 1), jnp.concatenate([near, far], 1)
    )
    own_first = side == core
    w_a = jnp.where(own_first, own_w, other_w)
    w_b = jnp.where(own_first, other_w, own_w)
    w_pair = jnp.stack([w_a, w_b])

    paired = bias_weight.reshape(-1, heads // 8, 2, QUAD).transpose(0, 1, 3, 2).reshape(-1, heads)
    tile = bias_tile_of(pair_repr, asym_id, rel_embed, pair_gain, paired)
    tile = tile.reshape(heads // 8, 1, QUAD, 2, tile_rows * tile_cols)
    tile = jnp.broadcast_to(tile, (heads // 8, 2, QUAD, 2, tile_rows * tile_cols))
    by_row = exchange(tile.reshape(rows, 2, tile_rows * tile_cols), "row")
    by_key = by_row.reshape(rows, 2, tile_rows, tile_cols).transpose(1, 3, 0, 2)
    by_key = by_key.reshape(2, tile_cols, total)
    keep = jnp.where(core == 0, by_key[0], by_key[1])
    got = lax.ppermute(jnp.where(core == 0, by_key[1], by_key[0]), "samp", swap)
    chip_keys = jnp.where(
        core == 0, jnp.concatenate([keep, got]), jnp.concatenate([got, keep])
    )
    col = lax.axis_index("col")

    def all_cols(block):
        size = block.shape[0]
        whole = jnp.zeros((cols * size, *block.shape[1:]), block.dtype)
        start = (0,) * (block.ndim - 1)
        whole = lax.dynamic_update_slice(whole, block, (col * size, *start))
        up = down = block
        for step in range(1, cols // 2 + 1):
            up = shifted(up, "col", 1)
            whole = lax.dynamic_update_slice(whole, up, ((col - step) % cols * size, *start))
            if step < cols // 2:
                down = shifted(down, "col", -1)
                whole = lax.dynamic_update_slice(whole, down, ((col + step) % cols * size, *start))
        return whole

    bias_a = all_cols(chip_keys)
    bias_b = lax.ppermute(bias_a, "samp", swap)
    biases = jnp.stack([bias_a, bias_b])

    normed = normalize(tokens.astype(jnp.float32), token_gain[0]).astype(jnp.bfloat16)
    half_rows = sample_count // 2 * token_rows
    halves = normed.reshape(2, half_rows, width)
    depth = out_weight.shape[1]
    slice_rows = depth // cols
    piece = lax.dynamic_slice_in_dim(out_weight[0], col * slice_rows, slice_rows, 0)
    same = jnp.concatenate([jnp.where(side == 0, halves[0], halves[1]), piece])
    cross = jnp.concatenate([jnp.where(side == 0, halves[1], halves[0]), piece])
    around = jnp.stack(
        [
            same,
            shifted(cross, "row", -QUAD),
            shifted(same, "row", 2 * QUAD),
            shifted(cross, "row", QUAD),
        ]
    )
    around = lax.dynamic_slice_in_dim(
        jnp.concatenate([around, around]), (quads - z // QUAD) % quads, quads, 0
    )
    gathered = jnp.broadcast_to(around[None], (QUAD, *around.shape))
    gathered = exchange(gathered, "row", adjacent)
    pieces = gathered[:, :, half_rows:].transpose(1, 0, 2, 3).reshape(-1, width)
    w_out = all_cols(pieces).reshape(cols, rows // 8, 2, QUAD, slice_rows, width)
    w_out = w_out.transpose(1, 3, 2, 0, 4, 5).reshape(width, width)
    gathered = gathered[:, :, :half_rows].reshape(
        QUAD, quads, sample_count // 2, token_rows, width
    )
    gathered = gathered.transpose(2, 1, 0, 3, 4).reshape(sample_count // 2, total, width)

    projected = jnp.einsum(
        "snc,hpcw->pshnw", gathered, w_pair, preferred_element_type=jnp.float32
    ).astype(jnp.bfloat16)
    query, key, value = projected[0], projected[1], projected[2]
    scores = (
        jnp.einsum("shjd,shid->shji", key, query, preferred_element_type=jnp.float32) * score_scale
        + biases[None]
    )
    mask = keymask[None, None, :, None]
    scores = jnp.where(mask, scores, -1e30)
    row_max = jnp.max(scores, axis=2, keepdims=True)
    weights = jnp.where(mask, jnp.exp(scores - row_max), 0.0)
    row_total = jnp.sum(weights, axis=2, keepdims=True)
    probs = (weights / row_total).astype(jnp.bfloat16)
    attended = jnp.einsum(
        "shji,shjd->sihd", probs, value, preferred_element_type=jnp.float32
    ).astype(jnp.bfloat16)
    attended = jnp.where(core == 0, attended, attended[:, :, ::-1])

    back = attended.reshape(sample_count // 2, rows, token_rows, 2 * HEAD_DIM)
    back = exchange(back.transpose(1, 0, 2, 3), "row")
    back = back.reshape(rows // 8, 2, QUAD, sample_count // 2, token_rows, 2 * HEAD_DIM)
    back = back.transpose(1, 3, 4, 0, 2, 5).reshape(sample_count * token_rows, width)
    update = jnp.dot(back, w_out, preferred_element_type=jnp.float32)
    return (
        tokens.astype(jnp.float32) + update.reshape(sample_count, token_rows, width)
    ).astype(jnp.bfloat16)


def solution(mesh):
    return jax.shard_map(
        per_device,
        mesh=mesh,
        in_specs=(
            P(("job", "row"), ("col", "samp"), None),
            P("job"),
            P("job"),
            P(),
            P(),
            P(),
            P(("job", "col", "samp"), "row", None),
            P(),
            P(None, None, None, "row"),
            P(None, "row", None),
        ),
        out_specs=P(("job", "col", "samp"), "row", None),
        check_vma=False,
    )
```

```python
import functools
import math

import jax
import jax.numpy as jnp
from jax import lax
from jax.experimental import pallas as pl
from jax.experimental.pallas import tpu as pltpu
from jax.sharding import PartitionSpec as P


HEAD_DIM = 48
QUAD = 4

epsilon = 1e-05


def normalize(values, gain_vector):
    average = jnp.mean(values, axis=-1, keepdims=True)
    centered = values - average
    variance = jnp.mean(centered * centered, axis=-1, keepdims=True)
    return centered * lax.rsqrt(variance + epsilon) * gain_vector


def exchange(blocks, axis, groups=None):
    return lax.all_to_all(
        blocks, axis, split_axis=0, concat_axis=0, axis_index_groups=groups, tiled=True
    )


def bias_tile_of(pair_repr, asym_id, rel_embed, pair_gain, bias_weight):
    tile_rows, tile_cols, channels = pair_repr.shape
    bin_count = rel_embed.shape[0]
    reach_max = bin_count // 2 - 1
    first_row = lax.axis_index("row") * tile_rows
    first_col = lax.axis_index(("col", "samp")) * tile_cols
    row_ids = first_row + jnp.arange(tile_rows, dtype=jnp.int32)
    col_ids = first_col + jnp.arange(tile_cols, dtype=jnp.int32)
    row_chain = lax.dynamic_slice_in_dim(asym_id, first_row, tile_rows, 0)
    col_chain = lax.dynamic_slice_in_dim(asym_id, first_col, tile_cols, 0)
    offset = jnp.clip(row_ids[:, None] - col_ids[None, :], -reach_max, reach_max) + reach_max
    bin_ids = jnp.where(row_chain[:, None] == col_chain[None, :], offset, bin_count - 1)
    onehot = (
        bin_ids.reshape(-1)[:, None] == jnp.arange(bin_count, dtype=jnp.int32)[None, :]
    ).astype(jnp.bfloat16)
    summed = pair_repr.reshape(-1, channels).astype(jnp.float32) + jnp.dot(
        onehot, rel_embed, preferred_element_type=jnp.float32
    )
    normed = normalize(summed, pair_gain).astype(jnp.bfloat16)
    projected = lax.dot_general(
        bias_weight, normed, (((0,), (1,)), ((), ())), preferred_element_type=jnp.float32
    )
    return projected


def attend_kernel(info_ref, blocks_ref, w_ref, bias_a_ref, bias_b_ref, out_ref, *, samples, scale):
    neighbours, quads, block_rows, _ = blocks_ref.shape
    token_rows = block_rows // samples
    total = bias_a_ref.shape[0]
    valid, quad, core = info_ref[0], info_ref[1], info_ref[2]
    key_ok = lax.broadcasted_iota(jnp.int32, (total, 1), 0) < valid
    dot = functools.partial(lax.dot_general, preferred_element_type=jnp.float32)
    for u in range(samples):
        x = jnp.concatenate(
            [
                blocks_ref[j, lax.rem(a - quad + quads, quads), pl.ds(u * token_rows, token_rows), :]
                for a in range(quads)
                for j in range(neighbours)
            ]
        )
        projected = dot(w_ref[...], x, (((1,), (1,)), ((), ()))).astype(jnp.bfloat16)
        outs = []
        for h, bias_ref in enumerate((bias_a_ref, bias_b_ref)):
            query, key, value = (
                projected[(h * 3 + p) * HEAD_DIM : (h * 3 + p + 1) * HEAD_DIM] for p in range(3)
            )
            scores = dot(key, query, (((0,), (0,)), ((), ()))) * scale + bias_ref[...]
            scores = jnp.where(key_ok, scores, -1e30)
            row_max = jnp.max(scores, axis=0, keepdims=True)
            weights = jnp.where(key_ok, jnp.exp(scores - row_max), 0.0)
            inverse = 1.0 / jnp.sum(weights, axis=0, keepdims=True)
            probs = (weights * inverse).astype(jnp.bfloat16)
            outs.append(dot(value, probs, (((1,), (0,)), ((), ()))))
        swapped = core == 1
        low = jnp.where(swapped, outs[1], outs[0])
        high = jnp.where(swapped, outs[0], outs[1])
        both = jnp.concatenate([low, high]).T.astype(jnp.bfloat16)
        for i in range(total // token_rows):
            out_ref[i, u] = both[i * token_rows : (i + 1) * token_rows]


def attend(info, blocks, w, bias_a, bias_b, samples):
    _, _, block_rows, width = blocks.shape
    total = bias_a.shape[0]
    token_rows = block_rows // samples
    vmem = pl.BlockSpec(memory_space=pltpu.VMEM)
    flops = 2 * samples * total * (width * w.shape[0] + 4 * total * HEAD_DIM)
    return pl.pallas_call(
        functools.partial(attend_kernel, samples=samples, scale=1.0 / math.sqrt(HEAD_DIM)),
        out_shape=jax.ShapeDtypeStruct(
            (total // token_rows, samples, token_rows, 2 * HEAD_DIM), jnp.bfloat16
        ),
        in_specs=[pl.BlockSpec(memory_space=pltpu.SMEM), vmem, vmem, vmem, vmem],
        out_specs=vmem,
        compiler_params=pltpu.CompilerParams(vmem_limit_bytes=48 * 1024 * 1024),
        cost_estimate=pl.CostEstimate(
            flops=flops, bytes_accessed=6 * 1024 * 1024, transcendentals=samples * 2 * total * total
        ),
        name="attend",
    )(info, blocks, w, bias_a, bias_b)


def per_device(
    pair_repr,
    asym_id,
    valid_len,
    rel_embed,
    pair_gain,
    bias_weight,
    tokens,
    token_gain,
    qkv_weight,
    out_weight,
):
    sample_count, token_rows, width = tokens.shape
    total = asym_id.shape[0]
    rows = lax.axis_size("row")
    cols = lax.axis_size("col")
    tile_rows, tile_cols, _ = pair_repr.shape
    heads = bias_weight.shape[1]
    quads = rows // QUAD
    adjacent = [[QUAD * a + b for b in range(QUAD)] for a in range(quads)]
    z = lax.axis_index("row")
    side = (z // QUAD) % 2
    core = lax.axis_index("samp")
    swap = [(0, 1), (1, 0)]

    def shifted(value, axis, by):
        size = lax.axis_size(axis)
        return lax.ppermute(value, axis, [(i, (i + by) % size) for i in range(size)])

    own_w = qkv_weight[0]
    half = width // 2
    part = lax.dynamic_slice_in_dim(own_w, core * half, half, 1)
    far = lax.ppermute(part, "row", [(i, i ^ QUAD) for i in range(rows)])
    near = lax.ppermute(far, "samp", swap)
    other_w = jnp.where(
        core == 0, jnp.concatenate([far, near], 1), jnp.concatenate([near, far], 1)
    )
    own_first = side == core
    w_a = jnp.where(own_first, own_w, other_w)
    w_b = jnp.where(own_first, other_w, own_w)
    w_pair = jnp.stack([w_a, w_b]).transpose(0, 1, 3, 2).reshape(-1, width)

    paired = bias_weight.reshape(-1, heads // 8, 2, QUAD).transpose(0, 1, 3, 2).reshape(-1, heads)
    tile = bias_tile_of(pair_repr, asym_id, rel_embed, pair_gain, paired)
    tile, tokens_in, part = lax.optimization_barrier((tile, tokens, part))
    normed = normalize(tokens_in.astype(jnp.float32), token_gain[0]).astype(jnp.bfloat16)
    half_samples = sample_count // 2
    half_rows = half_samples * token_rows
    halves = normed.reshape(2, half_rows, width)
    col = lax.axis_index("col")
    depth = out_weight.shape[1]
    slice_rows = depth // cols
    piece = lax.dynamic_slice_in_dim(out_weight[0], col * slice_rows, slice_rows, 0)
    same = jnp.concatenate([jnp.where(side == 0, halves[0], halves[1]), piece])
    cross = jnp.concatenate([jnp.where(side == 0, halves[1], halves[0]), piece])
    tile = tile.reshape(heads // 8, 1, QUAD, 2, tile_rows * tile_cols)
    tile = jnp.broadcast_to(tile, (heads // 8, 2, QUAD, 2, tile_rows * tile_cols))
    by_row = exchange(tile.reshape(rows, 2, tile_rows * tile_cols), "row")
    by_row, _, _ = lax.optimization_barrier((by_row, same, cross))
    by_key = by_row.reshape(rows, 2, tile_rows, tile_cols).transpose(1, 3, 0, 2)
    by_key = by_key.reshape(2, tile_cols, total)
    fanned = jnp.broadcast_to(by_key[None], (cols, *by_key.shape))
    bias_a = exchange(fanned.reshape(2 * cols, tile_cols, total), ("col", "samp"))
    bias_a = bias_a.reshape(total, total)
    bias_b = lax.ppermute(bias_a, "samp", swap)

    def all_cols(block):
        size = block.shape[0]
        whole = jnp.zeros((cols * size, *block.shape[1:]), block.dtype)
        start = (0,) * (block.ndim - 1)
        whole = lax.dynamic_update_slice(whole, block, (col * size, *start))
        up = down = block
        for step in range(1, cols // 2 + 1):
            up = shifted(up, "col", 1)
            whole = lax.dynamic_update_slice(whole, up, ((col - step) % cols * size, *start))
            if step < cols // 2:
                down = shifted(down, "col", -1)
                whole = lax.dynamic_update_slice(whole, down, ((col + step) % cols * size, *start))
        return whole

    opposite = shifted(same, "row", 2 * QUAD)
    before = shifted(cross, "row", QUAD)
    after = shifted(cross, "row", -QUAD)
    around = [same, after, opposite, before]
    blocks = jnp.stack([item[:half_rows] for item in around])
    blocks = jnp.broadcast_to(blocks[None], (QUAD, *blocks.shape))
    blocks = exchange(blocks, "row", adjacent)

    mine = jnp.concatenate([item[half_rows:] for item in around])
    turned = [mine]
    for by in range(1, QUAD):
        turns = [(i, i // QUAD * QUAD + (i - by) % QUAD) for i in range(rows)]
        turned.append(lax.ppermute(mine, "row", turns))
    turned = jnp.stack(turned).reshape(QUAD, quads, slice_rows, width)
    turned = lax.dynamic_slice_in_dim(
        jnp.concatenate([turned, turned]), (QUAD - z % QUAD) % QUAD, QUAD, 0
    )
    turned = lax.dynamic_slice_in_dim(
        jnp.concatenate([turned, turned], 1), (quads - z // QUAD) % quads, quads, 1
    )
    w_out = all_cols(turned.reshape(-1, width)).reshape(
        cols, QUAD, rows // 8, 2, slice_rows, width
    )
    w_out = w_out.transpose(2, 1, 3, 0, 4, 5).reshape(width, width)

    info = jnp.stack([valid_len[0], z // QUAD, core]).astype(jnp.int32)
    attended = attend(info, blocks, w_pair, bias_a, bias_b, half_samples)
    back = exchange(attended, "row")
    back = back.reshape(rows // 8, 2, QUAD, sample_count // 2, token_rows, 2 * HEAD_DIM)
    back = back.transpose(1, 3, 4, 0, 2, 5).reshape(sample_count * token_rows, width)
    update = jnp.dot(back, w_out, preferred_element_type=jnp.float32)
    return (
        tokens.astype(jnp.float32) + update.reshape(sample_count, token_rows, width)
    ).astype(jnp.bfloat16)


def solution(mesh):
    return jax.shard_map(
        per_device,
        mesh=mesh,
        in_specs=(
            P(("job", "row"), ("col", "samp"), None),
            P("job"),
            P("job"),
            P(),
            P(),
            P(),
            P(("job", "col", "samp"), "row", None),
            P(),
            P(None, None, None, "row"),
            P(None, "row", None),
        ),
        out_specs=P(("job", "col", "samp"), "row", None),
        check_vma=False,
    )
```

```python
import functools
import math

import jax
import jax.numpy as jnp
from jax import lax
from jax.experimental import pallas as pl
from jax.experimental.pallas import tpu as pltpu
from jax.sharding import PartitionSpec as P


HEAD_DIM = 48

epsilon = 1e-05


def normalize(values, gain_vector):
    average = jnp.mean(values, axis=-1, keepdims=True)
    centered = values - average
    variance = jnp.mean(centered * centered, axis=-1, keepdims=True)
    return centered * lax.rsqrt(variance + epsilon) * gain_vector


def exchange(blocks, axis, groups=None):
    return lax.all_to_all(
        blocks, axis, split_axis=0, concat_axis=0, axis_index_groups=groups, tiled=True
    )


def bias_tile_of(pair_repr, asym_id, rel_embed, pair_gain, bias_weight):
    tile_rows, tile_cols, channels = pair_repr.shape
    bin_count = rel_embed.shape[0]
    reach_max = bin_count // 2 - 1
    first_row = lax.axis_index("row") * tile_rows
    first_col = lax.axis_index(("col", "samp")) * tile_cols
    row_ids = first_row + jnp.arange(tile_rows, dtype=jnp.int32)
    col_ids = first_col + jnp.arange(tile_cols, dtype=jnp.int32)
    row_chain = lax.dynamic_slice_in_dim(asym_id, first_row, tile_rows, 0)
    col_chain = lax.dynamic_slice_in_dim(asym_id, first_col, tile_cols, 0)
    offset = jnp.clip(row_ids[:, None] - col_ids[None, :], -reach_max, reach_max) + reach_max
    bin_ids = jnp.where(row_chain[:, None] == col_chain[None, :], offset, bin_count - 1)
    onehot = (
        bin_ids.reshape(-1)[:, None] == jnp.arange(bin_count, dtype=jnp.int32)[None, :]
    ).astype(jnp.bfloat16)
    summed = pair_repr.reshape(-1, channels).astype(jnp.float32) + jnp.dot(
        onehot, rel_embed, preferred_element_type=jnp.float32
    )
    normed = normalize(summed, pair_gain).astype(jnp.bfloat16)
    projected = lax.dot_general(
        bias_weight, normed, (((0,), (1,)), ((), ())), preferred_element_type=jnp.float32
    )
    return projected


def attend_kernel(info_ref, blocks_ref, w_ref, bias_a_ref, bias_b_ref, out_ref, *, samples, scale):
    pairs, pair_rows, _ = blocks_ref.shape
    half_rows = pair_rows // 2
    token_rows = half_rows // samples
    total = bias_a_ref.shape[0]
    valid, side, core = info_ref[0], info_ref[1], info_ref[2]
    key_ok = lax.broadcasted_iota(jnp.int32, (total, 1), 0) < valid
    dot = functools.partial(lax.dot_general, preferred_element_type=jnp.float32)
    starts = [side * half_rows, (1 - side) * half_rows]
    for u in range(samples):
        x = jnp.concatenate(
            [
                blocks_ref[k, pl.ds(pl.multiple_of(start + u * token_rows, token_rows), token_rows), :]
                for k in range(pairs)
                for start in starts
            ]
        )
        projected = dot(w_ref[...], x, (((1,), (1,)), ((), ()))).astype(jnp.bfloat16)
        outs = []
        for h, bias_ref in enumerate((bias_a_ref, bias_b_ref)):
            query, key, value = (
                projected[(h * 3 + p) * HEAD_DIM : (h * 3 + p + 1) * HEAD_DIM] for p in range(3)
            )
            scores = dot(key, query, (((0,), (0,)), ((), ()))) * scale + bias_ref[...]
            scores = jnp.where(key_ok, scores, -1e30)
            row_max = jnp.max(scores, axis=0, keepdims=True)
            weights = jnp.where(key_ok, jnp.exp(scores - row_max), 0.0)
            inverse = 1.0 / jnp.sum(weights, axis=0, keepdims=True)
            probs = (weights * inverse).astype(jnp.bfloat16)
            outs.append(dot(value, probs, (((1,), (0,)), ((), ()))))
        swapped = core == 1
        low = jnp.where(swapped, outs[1], outs[0])
        high = jnp.where(swapped, outs[0], outs[1])
        both = jnp.concatenate([low, high]).T.astype(jnp.bfloat16)
        for i in range(total // token_rows):
            out_ref[i, u] = both[i * token_rows : (i + 1) * token_rows]


def attend(info, blocks, w, bias_a, bias_b, samples):
    width = blocks.shape[2]
    total = bias_a.shape[0]
    token_rows = blocks.shape[1] // 2 // samples
    vmem = pl.BlockSpec(memory_space=pltpu.VMEM)
    flops = 2 * samples * total * (width * w.shape[0] + 4 * total * HEAD_DIM)
    return pl.pallas_call(
        functools.partial(attend_kernel, samples=samples, scale=1.0 / math.sqrt(HEAD_DIM)),
        out_shape=jax.ShapeDtypeStruct(
            (total // token_rows, samples, token_rows, 2 * HEAD_DIM), jnp.bfloat16
        ),
        in_specs=[pl.BlockSpec(memory_space=pltpu.SMEM), vmem, vmem, vmem, vmem],
        out_specs=vmem,
        compiler_params=pltpu.CompilerParams(vmem_limit_bytes=48 * 1024 * 1024),
        cost_estimate=pl.CostEstimate(
            flops=flops, bytes_accessed=6 * 1024 * 1024, transcendentals=samples * 2 * total * total
        ),
        name="attend",
    )(info, blocks, w, bias_a, bias_b)


def per_device(
    pair_repr,
    asym_id,
    valid_len,
    rel_embed,
    pair_gain,
    bias_weight,
    tokens,
    token_gain,
    qkv_weight,
    out_weight,
):
    sample_count, token_rows, width = tokens.shape
    total = asym_id.shape[0]
    rows = lax.axis_size("row")
    cols = lax.axis_size("col")
    tile_rows, tile_cols, _ = pair_repr.shape
    pairs = rows // 2
    z = lax.axis_index("row")
    side = z % 2
    col = lax.axis_index("col")
    core = lax.axis_index("samp")
    swap = [(0, 1), (1, 0)]

    def shifted(value, axis, by):
        size = lax.axis_size(axis)
        return lax.ppermute(value, axis, [(i, (i + by) % size) for i in range(size)])

    def all_around(block, axis, by):
        count = lax.axis_size(axis) // by
        me = lax.axis_index(axis) // by
        whole = jnp.zeros((count, *block.shape), block.dtype)

        def put(whole, value, index):
            start = (index % count, *[0] * block.ndim)
            return lax.dynamic_update_slice(whole, value[None], start)

        whole = put(whole, block, me)
        up = down = block
        for step in range(1, count // 2 + 1):
            up = shifted(up, axis, by)
            if step < count // 2:
                down = shifted(down, axis, -by)
            if step < count // 2:
                whole = put(whole, down, me + step)
            whole = put(whole, up, me - step)
        return whole

    depth = out_weight.shape[1]
    slice_rows = depth // cols
    piece = lax.dynamic_slice_in_dim(out_weight[0], col * slice_rows, slice_rows, 0)
    pieces = exchange(jnp.broadcast_to(piece[None], (rows, *piece.shape)), "row")

    normed = normalize(tokens.astype(jnp.float32), token_gain[0]).astype(jnp.bfloat16)
    half_samples = sample_count // 2
    halves = normed.reshape(2, half_samples * token_rows, width)
    neighbour = [(i, i ^ 1) for i in range(rows)]
    given = lax.ppermute(jnp.where(side == 0, halves[1], halves[0]), "row", neighbour)
    block = jnp.concatenate([jnp.where(side == 0, halves[0], halves[1]), given])
    blocks = all_around(block, "row", 2)

    other_w = lax.ppermute(qkv_weight[0], "row", neighbour)
    own_first = side == core
    w_a = jnp.where(own_first, qkv_weight[0], other_w)
    w_b = jnp.where(own_first, other_w, qkv_weight[0])
    w_pair = jnp.stack([w_a, w_b]).transpose(0, 1, 3, 2).reshape(-1, width)

    tile = bias_tile_of(pair_repr, asym_id, rel_embed, pair_gain, bias_weight)
    tile = tile.reshape(pairs, 1, 2, tile_rows * tile_cols)
    tile = jnp.broadcast_to(tile, (pairs, 2, 2, tile_rows * tile_cols))
    by_row = exchange(tile.reshape(rows, 2, tile_rows * tile_cols), "row")
    by_key = by_row.reshape(rows, 2, tile_rows, tile_cols).transpose(1, 3, 0, 2)
    by_key = by_key.reshape(2, tile_cols, total)
    fanned = jnp.broadcast_to(by_key[None], (cols, *by_key.shape))
    bias_a = exchange(fanned.reshape(2 * cols, tile_cols, total), ("col", "samp"))
    bias_a = bias_a.reshape(total, total)
    bias_b = lax.ppermute(bias_a, "samp", swap)

    w_out = all_around(pieces, "col", 1)
    w_out = w_out.transpose(1, 0, 2, 3).reshape(width, width)

    info = jnp.stack([valid_len[0], side, core]).astype(jnp.int32)
    attended = attend(info, blocks, w_pair, bias_a, bias_b, half_samples)
    back = exchange(attended, "row")
    back = back.reshape(pairs, 2, half_samples, token_rows, 2 * HEAD_DIM)
    back = back.transpose(1, 2, 3, 0, 4).reshape(sample_count * token_rows, width)
    update = jnp.dot(back, w_out, preferred_element_type=jnp.float32)
    return (
        tokens.astype(jnp.float32) + update.reshape(sample_count, token_rows, width)
    ).astype(jnp.bfloat16)


def solution(mesh):
    return jax.shard_map(
        per_device,
        mesh=mesh,
        in_specs=(
            P(("job", "row"), ("col", "samp"), None),
            P("job"),
            P("job"),
            P(),
            P(),
            P(),
            P(("job", "col", "samp"), "row", None),
            P(),
            P(None, None, None, "row"),
            P(None, "row", None),
        ),
        out_specs=P(("job", "col", "samp"), "row", None),
        check_vma=False,
    )
```

```python
import functools
import math

import jax
import jax.numpy as jnp
from jax import lax
from jax.experimental import pallas as pl
from jax.experimental.pallas import tpu as pltpu
from jax.sharding import PartitionSpec as P


HEAD_DIM = 48

epsilon = 1e-05


def normalize(values, gain_vector):
    average = jnp.mean(values, axis=-1, keepdims=True)
    centered = values - average
    variance = jnp.mean(centered * centered, axis=-1, keepdims=True)
    return centered * lax.rsqrt(variance + epsilon) * gain_vector


def exchange(blocks, axis, groups=None):
    return lax.all_to_all(
        blocks, axis, split_axis=0, concat_axis=0, axis_index_groups=groups, tiled=True
    )


def bias_tile_of(pair_repr, asym_id, rel_embed, pair_gain, bias_weight):
    tile_rows, tile_cols, channels = pair_repr.shape
    bin_count = rel_embed.shape[0]
    reach_max = bin_count // 2 - 1
    first_row = lax.axis_index("row") * tile_rows
    first_col = lax.axis_index(("col", "samp")) * tile_cols
    row_ids = first_row + jnp.arange(tile_rows, dtype=jnp.int32)
    col_ids = first_col + jnp.arange(tile_cols, dtype=jnp.int32)
    row_chain = lax.dynamic_slice_in_dim(asym_id, first_row, tile_rows, 0)
    col_chain = lax.dynamic_slice_in_dim(asym_id, first_col, tile_cols, 0)
    offset = jnp.clip(row_ids[:, None] - col_ids[None, :], -reach_max, reach_max) + reach_max
    bin_ids = jnp.where(row_chain[:, None] == col_chain[None, :], offset, bin_count - 1)
    onehot = (
        bin_ids.reshape(-1)[:, None] == jnp.arange(bin_count, dtype=jnp.int32)[None, :]
    ).astype(jnp.bfloat16)
    summed = pair_repr.reshape(-1, channels).astype(jnp.float32) + jnp.dot(
        onehot, rel_embed, preferred_element_type=jnp.float32
    )
    normed = normalize(summed, pair_gain).astype(jnp.bfloat16)
    projected = lax.dot_general(
        bias_weight, normed, (((0,), (1,)), ((), ())), preferred_element_type=jnp.float32
    )
    return projected


def normalize_kernel(side_ref, tokens_ref, gain_ref, keep_ref, give_ref):
    samples, token_rows, width = tokens_ref.shape
    values = tokens_ref[...].reshape(samples * token_rows, width).astype(jnp.float32)
    normed = normalize(values, gain_ref[...]).astype(jnp.bfloat16)
    half = samples * token_rows // 2
    even = side_ref[0] == 0
    keep_ref[...] = jnp.where(even, normed[:half], normed[half:])
    give_ref[...] = jnp.where(even, normed[half:], normed[:half])


def normalized_halves(side, tokens, gain):
    samples, token_rows, width = tokens.shape
    half = jax.ShapeDtypeStruct((samples * token_rows // 2, width), jnp.bfloat16)
    vmem = pl.BlockSpec(memory_space=pltpu.VMEM)
    return pl.pallas_call(
        normalize_kernel,
        out_shape=(half, half),
        in_specs=[pl.BlockSpec(memory_space=pltpu.SMEM), vmem, vmem],
        out_specs=(vmem, vmem),
        cost_estimate=pl.CostEstimate(
            flops=10 * tokens.size, bytes_accessed=4 * tokens.size, transcendentals=0
        ),
        name="normalize",
    )(side, tokens, gain)


def attend_kernel(info_1_ref, info_2_ref, *refs, samples, scale):
    *block_refs, w_ref, bias_a_ref, bias_b_ref, out_ref, blocks_ref = refs
    pairs, pair_rows, _ = blocks_ref.shape
    half_rows = pair_rows // 2
    token_rows = half_rows // samples
    total = bias_a_ref.shape[0]
    valid, side, core, pair = info_1_ref[0], info_1_ref[1], info_2_ref[0], info_2_ref[1]
    key_ok = lax.broadcasted_iota(jnp.int32, (total, 1), 0) < valid
    dot = functools.partial(lax.dot_general, preferred_element_type=jnp.float32)
    for step, block_ref in enumerate(block_refs):
        blocks_ref[lax.rem(pair - step + pairs, pairs)] = block_ref[...]
    starts = [side * half_rows, (1 - side) * half_rows]
    for u in range(samples):
        x = jnp.concatenate(
            [
                blocks_ref[k, pl.ds(pl.multiple_of(start + u * token_rows, token_rows), token_rows), :]
                for k in range(pairs)
                for start in starts
            ]
        )
        projected = dot(w_ref[...], x, (((1,), (1,)), ((), ()))).astype(jnp.bfloat16)
        outs = []
        for h, bias_ref in enumerate((bias_a_ref, bias_b_ref)):
            query, key, value = (
                projected[(h * 3 + p) * HEAD_DIM : (h * 3 + p + 1) * HEAD_DIM] for p in range(3)
            )
            scores = dot(key, query, (((0,), (0,)), ((), ()))) * scale + bias_ref[...]
            scores = jnp.where(key_ok, scores, -1e30)
            row_max = jnp.max(scores, axis=0, keepdims=True)
            weights = jnp.where(key_ok, jnp.exp(scores - row_max), 0.0)
            inverse = 1.0 / jnp.sum(weights, axis=0, keepdims=True)
            probs = (weights * inverse).astype(jnp.bfloat16)
            outs.append(dot(value, probs, (((1,), (0,)), ((), ()))))
        swapped = core == 1
        low = jnp.where(swapped, outs[1], outs[0])
        high = jnp.where(swapped, outs[0], outs[1])
        both = jnp.concatenate([low, high]).T.astype(jnp.bfloat16)
        for i in range(total // token_rows):
            out_ref[i, u] = both[i * token_rows : (i + 1) * token_rows]


def attend(info_1, info_2, blocks, w, bias_a, bias_b, samples):
    pair_rows, width = blocks[0].shape
    total = bias_a.shape[0]
    token_rows = pair_rows // 2 // samples
    vmem = pl.BlockSpec(memory_space=pltpu.VMEM)
    flops = 2 * samples * total * (width * w.shape[0] + 4 * total * HEAD_DIM)
    return pl.pallas_call(
        functools.partial(attend_kernel, samples=samples, scale=1.0 / math.sqrt(HEAD_DIM)),
        out_shape=jax.ShapeDtypeStruct(
            (total // token_rows, samples, token_rows, 2 * HEAD_DIM), jnp.bfloat16
        ),
        in_specs=[pl.BlockSpec(memory_space=pltpu.SMEM)] * 2 + [vmem] * (len(blocks) + 3),
        out_specs=vmem,
        scratch_shapes=[pltpu.VMEM((len(blocks), pair_rows, width), jnp.bfloat16)],
        compiler_params=pltpu.CompilerParams(vmem_limit_bytes=48 * 1024 * 1024),
        cost_estimate=pl.CostEstimate(
            flops=flops, bytes_accessed=6 * 1024 * 1024, transcendentals=samples * 2 * total * total
        ),
        name="attend",
    )(info_1, info_2, *blocks, w, bias_a, bias_b)


def per_device(
    pair_repr,
    asym_id,
    valid_len,
    rel_embed,
    pair_gain,
    bias_weight,
    tokens,
    token_gain,
    qkv_weight,
    out_weight,
):
    sample_count, token_rows, width = tokens.shape
    total = asym_id.shape[0]
    rows = lax.axis_size("row")
    cols = lax.axis_size("col")
    tile_rows, tile_cols, _ = pair_repr.shape
    pairs = rows // 2
    z = lax.axis_index("row")
    side = z % 2
    col = lax.axis_index("col")
    core = lax.axis_index("samp")
    swap = [(0, 1), (1, 0)]
    def shifted(value, axis, by):
        size = lax.axis_size(axis)
        return lax.ppermute(value, axis, [(i, (i + by) % size) for i in range(size)])

    info_1 = jnp.stack([valid_len[0], side]).astype(jnp.int32)
    info_2 = jnp.stack([core, z // 2, valid_len[0]]).astype(jnp.int32)

    depth = out_weight.shape[1]
    slice_rows, half_width = depth // cols, width // 2
    piece = lax.dynamic_slice(
        out_weight[0], (col * slice_rows, core * half_width), (slice_rows, half_width)
    )
    pieces = exchange(jnp.broadcast_to(piece[None], (rows, *piece.shape)), "row")

    half_samples = sample_count // 2
    keep, give = normalized_halves(side.reshape(1), tokens, token_gain)
    neighbour = [(i, i ^ 1) for i in range(rows)]
    given = lax.ppermute(give, "row", neighbour)
    up = down = jnp.concatenate([keep, given])
    blocks = [up] + [None] * (pairs - 1)
    for step in range(1, pairs // 2 + 1):
        up = shifted(up, "row", 2)
        if step < pairs // 2:
            down = shifted(down, "row", -2)
            blocks[-step] = down
        blocks[step] = up

    other_w = lax.ppermute(qkv_weight[0], "row", neighbour)
    own_first = side == core
    w_a = jnp.where(own_first, qkv_weight[0], other_w)
    w_b = jnp.where(own_first, other_w, qkv_weight[0])
    w_pair = jnp.stack([w_a, w_b]).transpose(0, 1, 3, 2).reshape(-1, width)

    tile = bias_tile_of(pair_repr, asym_id, rel_embed, pair_gain, bias_weight)
    tile = tile.reshape(pairs, 1, 2, tile_rows * tile_cols)
    tile = jnp.broadcast_to(tile, (pairs, 2, 2, tile_rows * tile_cols))
    by_row = exchange(tile.reshape(rows, 2, tile_rows * tile_cols), "row")
    by_key = by_row.reshape(rows, 2, tile_rows, tile_cols).transpose(1, 3, 0, 2)
    by_key = by_key.reshape(2, tile_cols, total)
    fanned = jnp.broadcast_to(by_key[None], (cols, *by_key.shape))
    bias_a = exchange(fanned.reshape(2 * cols, tile_cols, total), ("col", "samp"))
    bias_a = bias_a.reshape(total, total)
    bias_b = lax.ppermute(bias_a, "samp", swap)

    w_half, bit, place = pieces, cols // 2, 0
    while bit:
        other = lax.ppermute(w_half, "col", [(i, i ^ bit) for i in range(cols)])
        low = (col & bit) == 0
        w_half = jnp.stack(
            [jnp.where(low, w_half, other), jnp.where(low, other, w_half)], axis=place
        )
        bit, place = bit // 2, place + 1
    other = lax.ppermute(w_half, "samp", swap)
    w_out = jnp.concatenate(
        [jnp.where(core == 0, w_half, other), jnp.where(core == 0, other, w_half)], axis=-1
    )
    w_out = w_out.reshape(cols, rows, slice_rows, width).transpose(1, 0, 2, 3)
    w_out = w_out.reshape(width, width)

    attended = attend(info_1, info_2, blocks, w_pair, bias_a, bias_b, half_samples)
    back = exchange(attended, "row")
    back = back.reshape(pairs, 2, half_samples, token_rows, 2 * HEAD_DIM)
    back = back.transpose(1, 2, 3, 0, 4).reshape(sample_count * token_rows, width)
    update = jnp.dot(back, w_out, preferred_element_type=jnp.float32)
    return (
        tokens.astype(jnp.float32) + update.reshape(sample_count, token_rows, width)
    ).astype(jnp.bfloat16)


def solution(mesh):
    return jax.shard_map(
        per_device,
        mesh=mesh,
        in_specs=(
            P(("job", "row"), ("col", "samp"), None),
            P("job"),
            P("job"),
            P(),
            P(),
            P(),
            P(("job", "col", "samp"), "row", None),
            P(),
            P(None, None, None, "row"),
            P(None, "row", None),
        ),
        out_specs=P(("job", "col", "samp"), "row", None),
        check_vma=False,
    )
```

```python
import functools
import math

import jax
import jax.numpy as jnp
from jax import lax
from jax.experimental import pallas as pl
from jax.experimental.pallas import tpu as pltpu
from jax.sharding import PartitionSpec as P


HEAD_DIM = 48

epsilon = 1e-05


def normalize(values, gain_vector):
    average = jnp.mean(values, axis=-1, keepdims=True)
    centered = values - average
    variance = jnp.mean(centered * centered, axis=-1, keepdims=True)
    return centered * lax.rsqrt(variance + epsilon) * gain_vector


def exchange(blocks, axis, groups=None):
    return lax.all_to_all(
        blocks, axis, split_axis=0, concat_axis=0, axis_index_groups=groups, tiled=True
    )


def bias_tile_of(pair_repr, asym_id, rel_embed, pair_gain, bias_weight):
    tile_rows, tile_cols, channels = pair_repr.shape
    bin_count = rel_embed.shape[0]
    reach_max = bin_count // 2 - 1
    first_row = lax.axis_index("row") * tile_rows
    first_col = lax.axis_index(("col", "samp")) * tile_cols
    row_ids = first_row + jnp.arange(tile_rows, dtype=jnp.int32)
    col_ids = first_col + jnp.arange(tile_cols, dtype=jnp.int32)
    row_chain = lax.dynamic_slice_in_dim(asym_id, first_row, tile_rows, 0)
    col_chain = lax.dynamic_slice_in_dim(asym_id, first_col, tile_cols, 0)
    offset = jnp.clip(row_ids[:, None] - col_ids[None, :], -reach_max, reach_max) + reach_max
    bin_ids = jnp.where(row_chain[:, None] == col_chain[None, :], offset, bin_count - 1)
    onehot = (
        bin_ids.reshape(-1)[:, None] == jnp.arange(bin_count, dtype=jnp.int32)[None, :]
    ).astype(jnp.bfloat16)
    summed = pair_repr.reshape(-1, channels).astype(jnp.float32) + jnp.dot(
        onehot, rel_embed, preferred_element_type=jnp.float32
    )
    normed = normalize(summed, pair_gain).astype(jnp.bfloat16)
    projected = lax.dot_general(
        bias_weight, normed, (((0,), (1,)), ((), ())), preferred_element_type=jnp.float32
    )
    return projected


def normalize_kernel(side_ref, tokens_ref, gain_ref, keep_ref, give_ref):
    samples, token_rows, width = tokens_ref.shape
    values = tokens_ref[...].reshape(samples * token_rows, width).astype(jnp.float32)
    normed = normalize(values, gain_ref[...]).astype(jnp.bfloat16)
    half = samples * token_rows // 2
    even = side_ref[0] == 0
    keep_ref[...] = jnp.where(even, normed[:half], normed[half:])
    give_ref[...] = jnp.where(even, normed[half:], normed[:half])


def normalized_halves(side, tokens, gain):
    samples, token_rows, width = tokens.shape
    half = jax.ShapeDtypeStruct((samples * token_rows // 2, width), jnp.bfloat16)
    vmem = pl.BlockSpec(memory_space=pltpu.VMEM)
    return pl.pallas_call(
        normalize_kernel,
        out_shape=(half, half),
        in_specs=[pl.BlockSpec(memory_space=pltpu.SMEM), vmem, vmem],
        out_specs=(vmem, vmem),
        cost_estimate=pl.CostEstimate(
            flops=10 * tokens.size, bytes_accessed=4 * tokens.size, transcendentals=0
        ),
        name="normalize",
    )(side, tokens, gain)


def attend_kernel(info_1_ref, info_2_ref, *refs, samples, scale):
    *block_refs, w_ref, bias_a_ref, bias_b_ref, out_ref, blocks_ref = refs
    pairs, pair_rows, _ = blocks_ref.shape
    half_rows = pair_rows // 2
    token_rows = half_rows // samples
    total = bias_a_ref.shape[0]
    valid, side, core, pair = info_1_ref[0], info_1_ref[1], info_2_ref[0], info_2_ref[1]
    key_ok = lax.broadcasted_iota(jnp.int32, (total, 1), 0) < valid
    dot = functools.partial(lax.dot_general, preferred_element_type=jnp.float32)
    for step, block_ref in enumerate(block_refs):
        blocks_ref[lax.rem(pair - step + pairs, pairs)] = block_ref[...]
    starts = [side * half_rows, (1 - side) * half_rows]
    for u in range(samples):
        x = jnp.concatenate(
            [
                blocks_ref[k, pl.ds(pl.multiple_of(start + u * token_rows, token_rows), token_rows), :]
                for k in range(pairs)
                for start in starts
            ]
        )
        projected = dot(w_ref[...], x, (((1,), (1,)), ((), ()))).astype(jnp.bfloat16)
        outs = []
        for h, bias_ref in enumerate((bias_a_ref, bias_b_ref)):
            query, key, value = (
                projected[(h * 3 + p) * HEAD_DIM : (h * 3 + p + 1) * HEAD_DIM] for p in range(3)
            )
            scores = dot(key, query, (((0,), (0,)), ((), ()))) * scale + bias_ref[...]
            scores = jnp.where(key_ok, scores, -1e30)
            row_max = jnp.max(scores, axis=0, keepdims=True)
            weights = jnp.where(key_ok, jnp.exp(scores - row_max), 0.0)
            inverse = 1.0 / jnp.sum(weights, axis=0, keepdims=True)
            probs = (weights * inverse).astype(jnp.bfloat16)
            outs.append(dot(value, probs, (((1,), (0,)), ((), ()))))
        swapped = core == 1
        low = jnp.where(swapped, outs[1], outs[0])
        high = jnp.where(swapped, outs[0], outs[1])
        both = jnp.concatenate([low, high]).T.astype(jnp.bfloat16)
        for i in range(total // token_rows):
            out_ref[i, u] = both[i * token_rows : (i + 1) * token_rows]


def attend(info_1, info_2, blocks, w, bias_a, bias_b, samples):
    pair_rows, width = blocks[0].shape
    total = bias_a.shape[0]
    token_rows = pair_rows // 2 // samples
    vmem = pl.BlockSpec(memory_space=pltpu.VMEM)
    flops = 2 * samples * total * (width * w.shape[0] + 4 * total * HEAD_DIM)
    return pl.pallas_call(
        functools.partial(attend_kernel, samples=samples, scale=1.0 / math.sqrt(HEAD_DIM)),
        out_shape=jax.ShapeDtypeStruct(
            (total // token_rows, samples, token_rows, 2 * HEAD_DIM), jnp.bfloat16
        ),
        in_specs=[pl.BlockSpec(memory_space=pltpu.SMEM)] * 2 + [vmem] * (len(blocks) + 3),
        out_specs=vmem,
        scratch_shapes=[pltpu.VMEM((len(blocks), pair_rows, width), jnp.bfloat16)],
        compiler_params=pltpu.CompilerParams(vmem_limit_bytes=48 * 1024 * 1024),
        cost_estimate=pl.CostEstimate(
            flops=flops, bytes_accessed=6 * 1024 * 1024, transcendentals=samples * 2 * total * total
        ),
        name="attend",
    )(info_1, info_2, *blocks, w, bias_a, bias_b)


def per_device(
    pair_repr,
    asym_id,
    valid_len,
    rel_embed,
    pair_gain,
    bias_weight,
    tokens,
    token_gain,
    qkv_weight,
    out_weight,
):
    sample_count, token_rows, width = tokens.shape
    total = asym_id.shape[0]
    rows = lax.axis_size("row")
    cols = lax.axis_size("col")
    tile_rows, tile_cols, _ = pair_repr.shape
    pairs = rows // 2
    z = lax.axis_index("row")
    side = z % 2
    col = lax.axis_index("col")
    core = lax.axis_index("samp")
    swap = [(0, 1), (1, 0)]
    def shifted(value, axis, by):
        size = lax.axis_size(axis)
        return lax.ppermute(value, axis, [(i, (i + by) % size) for i in range(size)])

    info_1 = jnp.stack([valid_len[0], side]).astype(jnp.int32)
    info_2 = jnp.stack([core, z // 2, valid_len[0]]).astype(jnp.int32)

    depth = out_weight.shape[1]
    slice_rows, half_width = depth // cols, width // 2
    piece = lax.dynamic_slice(
        out_weight[0], (col * slice_rows, core * half_width), (slice_rows, half_width)
    )
    pieces = exchange(jnp.broadcast_to(piece[None], (rows, *piece.shape)), "row")

    half_samples = sample_count // 2
    keep, give = normalized_halves(side.reshape(1), tokens, token_gain)
    neighbour = [(i, i ^ 1) for i in range(rows)]
    given = lax.ppermute(give, "row", neighbour)
    up = down = jnp.concatenate([keep, given])
    blocks = [up] + [None] * (pairs - 1)
    for step in range(1, pairs // 2 + 1):
        up = shifted(up, "row", 2)
        if step < pairs // 2:
            down = shifted(down, "row", -2)
            blocks[-step] = down
        blocks[step] = up

    other_w = lax.ppermute(qkv_weight[0], "row", neighbour)
    own_first = side == core
    w_a = jnp.where(own_first, qkv_weight[0], other_w)
    w_b = jnp.where(own_first, other_w, qkv_weight[0])
    w_pair = jnp.stack([w_a, w_b]).transpose(0, 1, 3, 2).reshape(-1, width)

    tile = bias_tile_of(pair_repr, asym_id, rel_embed, pair_gain, bias_weight)
    tile = tile.reshape(pairs, 1, 2, tile_rows * tile_cols)
    tile = jnp.broadcast_to(tile, (pairs, 2, 2, tile_rows * tile_cols))
    by_row = exchange(tile.reshape(rows, 2, tile_rows * tile_cols), "row")
    by_key = by_row.reshape(rows, 2, tile_rows, tile_cols).transpose(1, 3, 0, 2)
    by_key = by_key.reshape(2, tile_cols, total)
    fanned = jnp.broadcast_to(by_key[None], (cols, *by_key.shape))
    bias_a = exchange(fanned.reshape(2 * cols, tile_cols, total), ("col", "samp"))
    bias_a = bias_a.reshape(total, total)
    bias_b = lax.ppermute(bias_a, "samp", swap)

    pieces = pieces.reshape(1, rows * slice_rows, half_width)
    w_half = exchange(jnp.broadcast_to(pieces, (cols, *pieces.shape[1:])), "col")
    other = lax.ppermute(w_half, "samp", swap)
    w_out = jnp.concatenate(
        [jnp.where(core == 0, w_half, other), jnp.where(core == 0, other, w_half)], axis=-1
    )
    w_out = w_out.reshape(cols, rows, slice_rows, width).transpose(1, 0, 2, 3)
    w_out = w_out.reshape(width, width)

    attended = attend(info_1, info_2, blocks, w_pair, bias_a, bias_b, half_samples)
    back = exchange(attended, "row")
    back = back.reshape(pairs, 2, half_samples, token_rows, 2 * HEAD_DIM)
    back = back.transpose(1, 2, 3, 0, 4).reshape(sample_count * token_rows, width)
    update = jnp.dot(back, w_out, preferred_element_type=jnp.float32)
    return (
        tokens.astype(jnp.float32) + update.reshape(sample_count, token_rows, width)
    ).astype(jnp.bfloat16)


def solution(mesh):
    return jax.shard_map(
        per_device,
        mesh=mesh,
        in_specs=(
            P(("job", "row"), ("col", "samp"), None),
            P("job"),
            P("job"),
            P(),
            P(),
            P(),
            P(("job", "col", "samp"), "row", None),
            P(),
            P(None, None, None, "row"),
            P(None, "row", None),
        ),
        out_specs=P(("job", "col", "samp"), "row", None),
        check_vma=False,
    )
```

```python
import functools
import math

import jax
import jax.numpy as jnp
from jax import lax
from jax.experimental import pallas as pl
from jax.experimental.pallas import tpu as pltpu
from jax.sharding import PartitionSpec as P


HEAD_DIM = 48

epsilon = 1e-05


def normalize(values, gain_vector):
    average = jnp.mean(values, axis=-1, keepdims=True)
    centered = values - average
    variance = jnp.mean(centered * centered, axis=-1, keepdims=True)
    return centered * lax.rsqrt(variance + epsilon) * gain_vector


def exchange(blocks, axis, groups=None):
    return lax.all_to_all(
        blocks, axis, split_axis=0, concat_axis=0, axis_index_groups=groups, tiled=True
    )


def bias_tile_of(pair_repr, asym_id, rel_embed, pair_gain, bias_weight):
    tile_rows, tile_cols, channels = pair_repr.shape
    bin_count = rel_embed.shape[0]
    reach_max = bin_count // 2 - 1
    first_row = lax.axis_index("row") * tile_rows
    first_col = lax.axis_index(("col", "samp")) * tile_cols
    row_ids = first_row + jnp.arange(tile_rows, dtype=jnp.int32)
    col_ids = first_col + jnp.arange(tile_cols, dtype=jnp.int32)
    row_chain = lax.dynamic_slice_in_dim(asym_id, first_row, tile_rows, 0)
    col_chain = lax.dynamic_slice_in_dim(asym_id, first_col, tile_cols, 0)
    offset = jnp.clip(row_ids[:, None] - col_ids[None, :], -reach_max, reach_max) + reach_max
    bin_ids = jnp.where(row_chain[:, None] == col_chain[None, :], offset, bin_count - 1)
    onehot = (
        bin_ids.reshape(-1)[:, None] == jnp.arange(bin_count, dtype=jnp.int32)[None, :]
    ).astype(jnp.bfloat16)
    summed = pair_repr.reshape(-1, channels).astype(jnp.float32) + jnp.dot(
        onehot, rel_embed, preferred_element_type=jnp.float32
    )
    normed = normalize(summed, pair_gain).astype(jnp.bfloat16)
    projected = lax.dot_general(
        bias_weight, normed, (((0,), (1,)), ((), ())), preferred_element_type=jnp.float32
    )
    return projected


def normalize_kernel(side_ref, tokens_ref, gain_ref, keep_ref, give_ref):
    samples, token_rows, width = tokens_ref.shape
    values = tokens_ref[...].reshape(samples * token_rows, width).astype(jnp.float32)
    normed = normalize(values, gain_ref[...]).astype(jnp.bfloat16)
    half = samples * token_rows // 2
    even = side_ref[0] == 0
    keep_ref[...] = jnp.where(even, normed[:half], normed[half:])
    give_ref[...] = jnp.where(even, normed[half:], normed[:half])


def normalized_halves(side, tokens, gain):
    samples, token_rows, width = tokens.shape
    half = jax.ShapeDtypeStruct((samples * token_rows // 2, width), jnp.bfloat16)
    vmem = pl.BlockSpec(memory_space=pltpu.VMEM)
    return pl.pallas_call(
        normalize_kernel,
        out_shape=(half, half),
        in_specs=[pl.BlockSpec(memory_space=pltpu.SMEM), vmem, vmem],
        out_specs=(vmem, vmem),
        cost_estimate=pl.CostEstimate(
            flops=10 * tokens.size, bytes_accessed=4 * tokens.size, transcendentals=0
        ),
        name="normalize",
    )(side, tokens, gain)


def attend_kernel(info_1_ref, info_2_ref, *refs, samples, scale):
    *block_refs, w_ref, bias_a_ref, bias_b_ref, out_ref, blocks_ref = refs
    pairs, pair_rows, _ = blocks_ref.shape
    half_rows = pair_rows // 2
    token_rows = half_rows // samples
    total = bias_a_ref.shape[0]
    valid, side, core, pair = info_1_ref[0], info_1_ref[1], info_2_ref[0], info_2_ref[1]
    key_ok = lax.broadcasted_iota(jnp.int32, (total, 1), 0) < valid
    dot = functools.partial(lax.dot_general, preferred_element_type=jnp.float32)
    for step, block_ref in enumerate(block_refs):
        blocks_ref[lax.rem(pair - step + pairs, pairs)] = block_ref[...]
    starts = [side * half_rows, (1 - side) * half_rows]
    for u in range(samples):
        x = jnp.concatenate(
            [
                blocks_ref[k, pl.ds(pl.multiple_of(start + u * token_rows, token_rows), token_rows), :]
                for k in range(pairs)
                for start in starts
            ]
        )
        projected = dot(w_ref[...], x, (((1,), (1,)), ((), ()))).astype(jnp.bfloat16)
        outs = []
        for h, bias_ref in enumerate((bias_a_ref, bias_b_ref)):
            query, key, value = (
                projected[(h * 3 + p) * HEAD_DIM : (h * 3 + p + 1) * HEAD_DIM] for p in range(3)
            )
            scores = dot(key, query, (((0,), (0,)), ((), ()))) * scale + bias_ref[...]
            scores = jnp.where(key_ok, scores, -1e30)
            row_max = jnp.max(scores, axis=0, keepdims=True)
            weights = jnp.where(key_ok, jnp.exp(scores - row_max), 0.0)
            inverse = 1.0 / jnp.sum(weights, axis=0, keepdims=True)
            probs = (weights * inverse).astype(jnp.bfloat16)
            outs.append(dot(value, probs, (((1,), (0,)), ((), ()))))
        swapped = core == 1
        low = jnp.where(swapped, outs[1], outs[0])
        high = jnp.where(swapped, outs[0], outs[1])
        both = jnp.concatenate([low, high]).T.astype(jnp.bfloat16)
        for i in range(total // token_rows):
            out_ref[i, u] = both[i * token_rows : (i + 1) * token_rows]


def attend(info_1, info_2, blocks, w, bias_a, bias_b, samples):
    pair_rows, width = blocks[0].shape
    total = bias_a.shape[0]
    token_rows = pair_rows // 2 // samples
    vmem = pl.BlockSpec(memory_space=pltpu.VMEM)
    flops = 2 * samples * total * (width * w.shape[0] + 4 * total * HEAD_DIM)
    return pl.pallas_call(
        functools.partial(attend_kernel, samples=samples, scale=1.0 / math.sqrt(HEAD_DIM)),
        out_shape=jax.ShapeDtypeStruct(
            (total // token_rows, samples, token_rows, 2 * HEAD_DIM), jnp.bfloat16
        ),
        in_specs=[pl.BlockSpec(memory_space=pltpu.SMEM)] * 2 + [vmem] * (len(blocks) + 3),
        out_specs=vmem,
        scratch_shapes=[pltpu.VMEM((len(blocks), pair_rows, width), jnp.bfloat16)],
        compiler_params=pltpu.CompilerParams(vmem_limit_bytes=48 * 1024 * 1024),
        cost_estimate=pl.CostEstimate(
            flops=flops, bytes_accessed=6 * 1024 * 1024, transcendentals=samples * 2 * total * total
        ),
        name="attend",
    )(info_1, info_2, *blocks, w, bias_a, bias_b)


def per_device(
    pair_repr,
    asym_id,
    valid_len,
    rel_embed,
    pair_gain,
    bias_weight,
    tokens,
    token_gain,
    qkv_weight,
    out_weight,
):
    sample_count, token_rows, width = tokens.shape
    total = asym_id.shape[0]
    rows = lax.axis_size("row")
    cols = lax.axis_size("col")
    tile_rows, tile_cols, _ = pair_repr.shape
    pairs = rows // 2
    z = lax.axis_index("row")
    side = z % 2
    col = lax.axis_index("col")
    core = lax.axis_index("samp")
    swap = [(0, 1), (1, 0)]
    def shifted(value, axis, by):
        size = lax.axis_size(axis)
        return lax.ppermute(value, axis, [(i, (i + by) % size) for i in range(size)])

    info_1 = jnp.stack([valid_len[0], side]).astype(jnp.int32)
    info_2 = jnp.stack([core, z // 2, valid_len[0]]).astype(jnp.int32)

    depth = out_weight.shape[1]
    slice_rows, half_width = depth // cols, width // 2
    piece = lax.dynamic_slice(
        out_weight[0], (col * slice_rows, core * half_width), (slice_rows, half_width)
    )

    half_samples = sample_count // 2
    keep, give = normalized_halves(side.reshape(1), tokens, token_gain)
    neighbour = [(i, i ^ 1) for i in range(rows)]
    given = lax.ppermute(give, "row", neighbour)
    up = down = jnp.concatenate([keep, given])
    blocks = [up] + [None] * (pairs - 1)
    for step in range(1, pairs // 2 + 1):
        up = shifted(up, "row", 2)
        if step < pairs // 2:
            down = shifted(down, "row", -2)
            blocks[-step] = down
        blocks[step] = up

    other_w = lax.ppermute(qkv_weight[0], "row", neighbour)
    own_first = side == core
    w_a = jnp.where(own_first, qkv_weight[0], other_w)
    w_b = jnp.where(own_first, other_w, qkv_weight[0])
    w_pair = jnp.stack([w_a, w_b]).transpose(0, 1, 3, 2).reshape(-1, width)

    tile = bias_tile_of(pair_repr, asym_id, rel_embed, pair_gain, bias_weight)
    lanes = 128
    tile = tile.reshape(pairs, 1, -1, lanes)
    tile_lines = tile.shape[2]
    tile = jnp.broadcast_to(tile, (pairs, 2, tile_lines, lanes)).reshape(rows, tile_lines, lanes)
    piece = piece.astype(jnp.float32).reshape(1, -1, lanes)
    piece = jnp.broadcast_to(piece, (rows, *piece.shape[1:]))
    by_row = exchange(jnp.concatenate([tile, piece], 1), "row")
    pieces = by_row[:, tile_lines:].astype(jnp.bfloat16)
    by_key = by_row[:, :tile_lines].reshape(rows, 2, tile_rows, tile_cols).transpose(1, 3, 0, 2)
    by_key = by_key.reshape(2, tile_cols, total)
    fanned = jnp.broadcast_to(by_key[None], (cols, *by_key.shape))
    bias_a = exchange(fanned.reshape(2 * cols, tile_cols, total), ("col", "samp"))
    bias_a = bias_a.reshape(total, total)
    bias_b = lax.ppermute(bias_a, "samp", swap)

    w_half = pieces.reshape(rows * slice_rows, half_width)
    bit, place = cols // 2, 0
    while bit:
        other = lax.ppermute(w_half, "col", [(i, i ^ bit) for i in range(cols)])
        low = (col & bit) == 0
        w_half = jnp.stack(
            [jnp.where(low, w_half, other), jnp.where(low, other, w_half)], axis=place
        )
        bit, place = bit // 2, place + 1
    other = lax.ppermute(w_half, "samp", swap)
    w_out = jnp.concatenate(
        [jnp.where(core == 0, w_half, other), jnp.where(core == 0, other, w_half)], axis=-1
    )
    w_out = w_out.reshape(cols, rows, slice_rows, width).transpose(1, 0, 2, 3)
    w_out = w_out.reshape(width, width)

    attended = attend(info_1, info_2, blocks, w_pair, bias_a, bias_b, half_samples)
    back = exchange(attended, "row")
    back = back.reshape(pairs, 2, half_samples, token_rows, 2 * HEAD_DIM)
    back = back.transpose(1, 2, 3, 0, 4).reshape(sample_count * token_rows, width)
    update = jnp.dot(back, w_out, preferred_element_type=jnp.float32)
    return (
        tokens.astype(jnp.float32) + update.reshape(sample_count, token_rows, width)
    ).astype(jnp.bfloat16)


def solution(mesh):
    return jax.shard_map(
        per_device,
        mesh=mesh,
        in_specs=(
            P(("job", "row"), ("col", "samp"), None),
            P("job"),
            P("job"),
            P(),
            P(),
            P(),
            P(("job", "col", "samp"), "row", None),
            P(),
            P(None, None, None, "row"),
            P(None, "row", None),
        ),
        out_specs=P(("job", "col", "samp"), "row", None),
        check_vma=False,
    )
```

```python
import functools
import math

import jax
import jax.numpy as jnp
from jax import lax
from jax.experimental import pallas as pl
from jax.experimental.pallas import tpu as pltpu
from jax.sharding import PartitionSpec as P


HEAD_DIM = 48

epsilon = 1e-05


def normalize(values, gain_vector):
    average = jnp.mean(values, axis=-1, keepdims=True)
    centered = values - average
    variance = jnp.mean(centered * centered, axis=-1, keepdims=True)
    return centered * lax.rsqrt(variance + epsilon) * gain_vector


def exchange(blocks, axis, groups=None):
    return lax.all_to_all(
        blocks, axis, split_axis=0, concat_axis=0, axis_index_groups=groups, tiled=True
    )


def bias_tile_of(pair_repr, asym_id, rel_embed, pair_gain, bias_weight):
    tile_rows, tile_cols, channels = pair_repr.shape
    bin_count = rel_embed.shape[0]
    reach_max = bin_count // 2 - 1
    first_row = lax.axis_index("row") * tile_rows
    first_col = lax.axis_index(("col", "samp")) * tile_cols
    row_ids = first_row + jnp.arange(tile_rows, dtype=jnp.int32)
    col_ids = first_col + jnp.arange(tile_cols, dtype=jnp.int32)
    row_chain = lax.dynamic_slice_in_dim(asym_id, first_row, tile_rows, 0)
    col_chain = lax.dynamic_slice_in_dim(asym_id, first_col, tile_cols, 0)
    offset = jnp.clip(row_ids[:, None] - col_ids[None, :], -reach_max, reach_max) + reach_max
    bin_ids = jnp.where(row_chain[:, None] == col_chain[None, :], offset, bin_count - 1)
    onehot = (
        bin_ids.reshape(-1)[:, None] == jnp.arange(bin_count, dtype=jnp.int32)[None, :]
    ).astype(jnp.bfloat16)
    summed = pair_repr.reshape(-1, channels).astype(jnp.float32) + jnp.dot(
        onehot, rel_embed, preferred_element_type=jnp.float32
    )
    normed = normalize(summed, pair_gain).astype(jnp.bfloat16)
    projected = lax.dot_general(
        bias_weight, normed, (((0,), (1,)), ((), ())), preferred_element_type=jnp.float32
    )
    return projected


def normalize_kernel(side_ref, tokens_ref, gain_ref, keep_ref, give_ref):
    samples, token_rows, width = tokens_ref.shape
    values = tokens_ref[...].reshape(samples * token_rows, width).astype(jnp.float32)
    normed = normalize(values, gain_ref[...]).astype(jnp.bfloat16)
    half = samples * token_rows // 2
    even = side_ref[0] == 0
    keep_ref[...] = jnp.where(even, normed[:half], normed[half:])
    give_ref[...] = jnp.where(even, normed[half:], normed[:half])


def normalized_halves(side, tokens, gain):
    samples, token_rows, width = tokens.shape
    half = jax.ShapeDtypeStruct((samples * token_rows // 2, width), jnp.bfloat16)
    vmem = pl.BlockSpec(memory_space=pltpu.VMEM)
    return pl.pallas_call(
        normalize_kernel,
        out_shape=(half, half),
        in_specs=[pl.BlockSpec(memory_space=pltpu.SMEM), vmem, vmem],
        out_specs=(vmem, vmem),
        cost_estimate=pl.CostEstimate(
            flops=10 * tokens.size, bytes_accessed=4 * tokens.size, transcendentals=0
        ),
        name="normalize",
    )(side, tokens, gain)


def attend_kernel(info_1_ref, info_2_ref, *refs, samples, scale):
    *block_refs, w_ref, bias_a_ref, bias_b_ref, out_ref, blocks_ref = refs
    pairs, pair_rows, _ = blocks_ref.shape
    half_rows = pair_rows // 2
    token_rows = half_rows // samples
    total = bias_a_ref.shape[0]
    valid, side, core, pair = info_1_ref[0], info_1_ref[1], info_2_ref[0], info_2_ref[1]
    key_ok = lax.broadcasted_iota(jnp.int32, (total, 1), 0) < valid
    dot = functools.partial(lax.dot_general, preferred_element_type=jnp.float32)
    for step, block_ref in enumerate(block_refs):
        blocks_ref[lax.rem(pair - step + pairs, pairs)] = block_ref[...]
    starts = [side * half_rows, (1 - side) * half_rows]
    for u in range(samples):
        x = jnp.concatenate(
            [
                blocks_ref[k, pl.ds(pl.multiple_of(start + u * token_rows, token_rows), token_rows), :]
                for k in range(pairs)
                for start in starts
            ]
        )
        projected = dot(w_ref[...], x, (((1,), (1,)), ((), ()))).astype(jnp.bfloat16)
        outs = []
        for h, bias_ref in enumerate((bias_a_ref, bias_b_ref)):
            query, key, value = (
                projected[(h * 3 + p) * HEAD_DIM : (h * 3 + p + 1) * HEAD_DIM] for p in range(3)
            )
            scores = dot(key, query, (((0,), (0,)), ((), ()))) * scale + bias_ref[...]
            scores = jnp.where(key_ok, scores, -1e30)
            row_max = jnp.max(scores, axis=0, keepdims=True)
            weights = jnp.where(key_ok, jnp.exp(scores - row_max), 0.0)
            inverse = 1.0 / jnp.sum(weights, axis=0, keepdims=True)
            probs = (weights * inverse).astype(jnp.bfloat16)
            outs.append(dot(value, probs, (((1,), (0,)), ((), ()))))
        swapped = core == 1
        low = jnp.where(swapped, outs[1], outs[0])
        high = jnp.where(swapped, outs[0], outs[1])
        both = jnp.concatenate([low, high]).T.astype(jnp.bfloat16)
        for i in range(total // token_rows):
            out_ref[i, u] = both[i * token_rows : (i + 1) * token_rows]


def attend(info_1, info_2, blocks, w, bias_a, bias_b, samples):
    pair_rows, width = blocks[0].shape
    total = bias_a.shape[0]
    token_rows = pair_rows // 2 // samples
    vmem = pl.BlockSpec(memory_space=pltpu.VMEM)
    flops = 2 * samples * total * (width * w.shape[0] + 4 * total * HEAD_DIM)
    return pl.pallas_call(
        functools.partial(attend_kernel, samples=samples, scale=1.0 / math.sqrt(HEAD_DIM)),
        out_shape=jax.ShapeDtypeStruct(
            (total // token_rows, samples, token_rows, 2 * HEAD_DIM), jnp.bfloat16
        ),
        in_specs=[pl.BlockSpec(memory_space=pltpu.SMEM)] * 2 + [vmem] * (len(blocks) + 3),
        out_specs=vmem,
        scratch_shapes=[pltpu.VMEM((len(blocks), pair_rows, width), jnp.bfloat16)],
        compiler_params=pltpu.CompilerParams(vmem_limit_bytes=48 * 1024 * 1024),
        cost_estimate=pl.CostEstimate(
            flops=flops, bytes_accessed=6 * 1024 * 1024, transcendentals=samples * 2 * total * total
        ),
        name="attend",
    )(info_1, info_2, *blocks, w, bias_a, bias_b)


def per_device(
    pair_repr,
    asym_id,
    valid_len,
    rel_embed,
    pair_gain,
    bias_weight,
    tokens,
    token_gain,
    qkv_weight,
    out_weight,
):
    sample_count, token_rows, width = tokens.shape
    total = asym_id.shape[0]
    rows = lax.axis_size("row")
    cols = lax.axis_size("col")
    tile_rows, tile_cols, _ = pair_repr.shape
    pairs = rows // 2
    z = lax.axis_index("row")
    side = z % 2
    col = lax.axis_index("col")
    core = lax.axis_index("samp")
    swap = [(0, 1), (1, 0)]
    def shifted(value, axis, by):
        size = lax.axis_size(axis)
        return lax.ppermute(value, axis, [(i, (i + by) % size) for i in range(size)])

    info_1 = jnp.stack([valid_len[0], side]).astype(jnp.int32)
    info_2 = jnp.stack([core, z // 2, valid_len[0]]).astype(jnp.int32)

    depth = out_weight.shape[1]
    slice_rows, half_width = depth // cols, width // 2
    piece = lax.dynamic_slice(
        out_weight[0], (col * slice_rows, core * half_width), (slice_rows, half_width)
    )

    half_samples = sample_count // 2
    keep, give = normalized_halves(side.reshape(1), tokens, token_gain)
    neighbour = [(i, i ^ 1) for i in range(rows)]
    given = lax.ppermute(give, "row", neighbour)
    up = down = jnp.concatenate([keep, given])
    blocks = [up] + [None] * (pairs - 1)
    for step in range(1, pairs // 2 + 1):
        up = shifted(up, "row", 2)
        if step < pairs // 2:
            down = shifted(down, "row", -2)
            blocks[-step] = down
        blocks[step] = up

    other_w = lax.ppermute(qkv_weight[0], "row", neighbour)
    own_first = side == core
    w_a = jnp.where(own_first, qkv_weight[0], other_w)
    w_b = jnp.where(own_first, other_w, qkv_weight[0])
    w_pair = jnp.stack([w_a, w_b]).transpose(0, 1, 3, 2).reshape(-1, width)

    tile = bias_tile_of(pair_repr, asym_id, rel_embed, pair_gain, bias_weight)
    lanes = 128
    tile = tile.reshape(pairs, 1, -1, lanes)
    tile_lines = tile.shape[2]
    tile = jnp.broadcast_to(tile, (pairs, 2, tile_lines, lanes)).reshape(rows, tile_lines, lanes)
    by_row = exchange(tile, "row")
    by_key = by_row.reshape(rows, 2, tile_rows, tile_cols).transpose(1, 3, 0, 2)
    pieces = exchange(jnp.broadcast_to(piece[None], (rows, *piece.shape)), "row")
    by_key = by_key.reshape(2, tile_cols, total)
    fanned = jnp.broadcast_to(by_key[None], (cols, *by_key.shape))
    bias_a = exchange(fanned.reshape(2 * cols, tile_cols, total), ("col", "samp"))
    bias_a = bias_a.reshape(total, total)
    bias_b = lax.ppermute(bias_a, "samp", swap)

    w_half = pieces.reshape(rows * slice_rows, half_width)
    bit, place = cols // 2, 0
    while bit:
        other = lax.ppermute(w_half, "col", [(i, i ^ bit) for i in range(cols)])
        low = (col & bit) == 0
        w_half = jnp.stack(
            [jnp.where(low, w_half, other), jnp.where(low, other, w_half)], axis=place
        )
        bit, place = bit // 2, place + 1
    other = lax.ppermute(w_half, "samp", swap)
    w_out = jnp.concatenate(
        [jnp.where(core == 0, w_half, other), jnp.where(core == 0, other, w_half)], axis=-1
    )
    w_out = w_out.reshape(cols, rows, slice_rows, width).transpose(1, 0, 2, 3)
    w_out = w_out.reshape(width, width)

    attended = attend(info_1, info_2, blocks, w_pair, bias_a, bias_b, half_samples)
    back = exchange(attended, "row")
    back = back.reshape(pairs, 2, half_samples, token_rows, 2 * HEAD_DIM)
    back = back.transpose(1, 2, 3, 0, 4).reshape(sample_count * token_rows, width)
    update = jnp.dot(back, w_out, preferred_element_type=jnp.float32)
    return (
        tokens.astype(jnp.float32) + update.reshape(sample_count, token_rows, width)
    ).astype(jnp.bfloat16)


def solution(mesh):
    return jax.shard_map(
        per_device,
        mesh=mesh,
        in_specs=(
            P(("job", "row"), ("col", "samp"), None),
            P("job"),
            P("job"),
            P(),
            P(),
            P(),
            P(("job", "col", "samp"), "row", None),
            P(),
            P(None, None, None, "row"),
            P(None, "row", None),
        ),
        out_specs=P(("job", "col", "samp"), "row", None),
        check_vma=False,
    )
```

```python
import functools
import math

import jax
import jax.numpy as jnp
from jax import lax
from jax.experimental import pallas as pl
from jax.experimental.pallas import tpu as pltpu
from jax.sharding import PartitionSpec as P


HEAD_DIM = 48

epsilon = 1e-05


def normalize(values, gain_vector):
    average = jnp.mean(values, axis=-1, keepdims=True)
    centered = values - average
    variance = jnp.mean(centered * centered, axis=-1, keepdims=True)
    return centered * lax.rsqrt(variance + epsilon) * gain_vector


def exchange(blocks, axis, groups=None):
    return lax.all_to_all(
        blocks, axis, split_axis=0, concat_axis=0, axis_index_groups=groups, tiled=True
    )


def bias_tile_of(pair_repr, asym_id, rel_embed, pair_gain, bias_weight):
    tile_rows, tile_cols, channels = pair_repr.shape
    bin_count = rel_embed.shape[0]
    reach_max = bin_count // 2 - 1
    first_row = lax.axis_index("row") * tile_rows
    first_col = lax.axis_index(("col", "samp")) * tile_cols
    row_ids = first_row + jnp.arange(tile_rows, dtype=jnp.int32)
    col_ids = first_col + jnp.arange(tile_cols, dtype=jnp.int32)
    row_chain = lax.dynamic_slice_in_dim(asym_id, first_row, tile_rows, 0)
    col_chain = lax.dynamic_slice_in_dim(asym_id, first_col, tile_cols, 0)
    offset = jnp.clip(row_ids[:, None] - col_ids[None, :], -reach_max, reach_max) + reach_max
    bin_ids = jnp.where(row_chain[:, None] == col_chain[None, :], offset, bin_count - 1)
    onehot = (
        bin_ids.reshape(-1)[:, None] == jnp.arange(bin_count, dtype=jnp.int32)[None, :]
    ).astype(jnp.bfloat16)
    summed = pair_repr.reshape(-1, channels).astype(jnp.float32) + jnp.dot(
        onehot, rel_embed, preferred_element_type=jnp.float32
    )
    normed = normalize(summed, pair_gain).astype(jnp.bfloat16)
    projected = lax.dot_general(
        bias_weight, normed, (((0,), (1,)), ((), ())), preferred_element_type=jnp.float32
    )
    return projected


def normalize_kernel(side_ref, tokens_ref, gain_ref, keep_ref, give_ref):
    samples, token_rows, width = tokens_ref.shape
    values = tokens_ref[...].reshape(samples * token_rows, width).astype(jnp.float32)
    normed = normalize(values, gain_ref[...]).astype(jnp.bfloat16)
    half = samples * token_rows // 2
    even = side_ref[0] == 0
    keep_ref[...] = jnp.where(even, normed[:half], normed[half:])
    give_ref[...] = jnp.where(even, normed[half:], normed[:half])


def normalized_halves(side, tokens, gain):
    samples, token_rows, width = tokens.shape
    half = jax.ShapeDtypeStruct((samples * token_rows // 2, width), jnp.bfloat16)
    vmem = pl.BlockSpec(memory_space=pltpu.VMEM)
    return pl.pallas_call(
        normalize_kernel,
        out_shape=(half, half),
        in_specs=[pl.BlockSpec(memory_space=pltpu.SMEM), vmem, vmem],
        out_specs=(vmem, vmem),
        cost_estimate=pl.CostEstimate(
            flops=10 * tokens.size, bytes_accessed=4 * tokens.size, transcendentals=0
        ),
        name="normalize",
    )(side, tokens, gain)


def attend_kernel(info_1_ref, info_2_ref, *refs, samples, scale):
    *block_refs, w_ref, bias_a_ref, bias_b_ref, out_ref, blocks_ref = refs
    pairs, pair_rows, _ = blocks_ref.shape
    half_rows = pair_rows // 2
    token_rows = half_rows // samples
    total = bias_a_ref.shape[0]
    valid, side, core, pair = info_1_ref[0], info_1_ref[1], info_2_ref[0], info_2_ref[1]
    key_ok = lax.broadcasted_iota(jnp.int32, (total, 1), 0) < valid
    dot = functools.partial(lax.dot_general, preferred_element_type=jnp.float32)
    for step, block_ref in enumerate(block_refs):
        blocks_ref[lax.rem(pair - step + pairs, pairs)] = block_ref[...]
    swapped = core == 1
    ordered = [[], []]
    starts = [side * half_rows, (1 - side) * half_rows]
    for u in range(samples):
        x = jnp.concatenate(
            [
                blocks_ref[k, pl.ds(pl.multiple_of(start + u * token_rows, token_rows), token_rows), :]
                for k in range(pairs)
                for start in starts
            ]
        )
        projected = dot(w_ref[...], x, (((1,), (1,)), ((), ()))).astype(jnp.bfloat16)
        outs = []
        for h, bias_ref in enumerate((bias_a_ref, bias_b_ref)):
            query, key, value = (
                projected[(h * 3 + p) * HEAD_DIM : (h * 3 + p + 1) * HEAD_DIM] for p in range(3)
            )
            scores = dot(key, query, (((0,), (0,)), ((), ()))) * scale + bias_ref[...]
            scores = jnp.where(key_ok, scores, -1e30)
            row_max = jnp.max(scores, axis=0, keepdims=True)
            weights = jnp.where(key_ok, jnp.exp(scores - row_max), 0.0)
            inverse = 1.0 / jnp.sum(weights, axis=0, keepdims=True)
            probs = (weights * inverse).astype(jnp.bfloat16)
            outs.append(dot(value, probs, (((1,), (0,)), ((), ()))))
        ordered[0].append(jnp.where(swapped, outs[1], outs[0]))
        ordered[1].append(jnp.where(swapped, outs[0], outs[1]))
    for i in range(total // token_rows):
        at = slice(i * token_rows, (i + 1) * token_rows)
        out_ref[i] = jnp.concatenate(
            [value[:, at] for head in ordered for value in head], axis=1
        ).astype(jnp.bfloat16)


def output_kernel(back_ref, w_ref, tokens_ref, out_ref):
    rows, _, lanes = back_ref.shape
    half_samples = tokens_ref.shape[0] // 2
    half = lanes // 2
    for side in range(2):
        pieces = []
        for k in range(rows // 2):
            block = back_ref[2 * k + side].astype(jnp.float32)
            pieces += [block[:, :half], block[:, half:]]
        attended = jnp.concatenate(pieces).astype(jnp.bfloat16)
        update = lax.dot_general(
            attended, w_ref[...], (((0,), (0,)), ((), ())), preferred_element_type=jnp.float32
        )
        samples = pl.ds(side * half_samples, half_samples)
        before = tokens_ref[samples].astype(jnp.float32)
        out_ref[samples] = (before + update.reshape(before.shape)).astype(jnp.bfloat16)


def output(back, w_out, tokens):
    vmem = pl.BlockSpec(memory_space=pltpu.VMEM)
    return pl.pallas_call(
        output_kernel,
        out_shape=jax.ShapeDtypeStruct(tokens.shape, jnp.bfloat16),
        in_specs=[vmem, vmem, vmem],
        out_specs=vmem,
        cost_estimate=pl.CostEstimate(
            flops=2 * tokens.size * w_out.shape[0], bytes_accessed=4 * 1024 * 1024, transcendentals=0
        ),
        name="output",
    )(back, w_out, tokens)


def attend(info_1, info_2, blocks, w, bias_a, bias_b, samples):
    pair_rows, width = blocks[0].shape
    total = bias_a.shape[0]
    token_rows = pair_rows // 2 // samples
    vmem = pl.BlockSpec(memory_space=pltpu.VMEM)
    flops = 2 * samples * total * (width * w.shape[0] + 4 * total * HEAD_DIM)
    return pl.pallas_call(
        functools.partial(attend_kernel, samples=samples, scale=1.0 / math.sqrt(HEAD_DIM)),
        out_shape=jax.ShapeDtypeStruct(
            (total // token_rows, HEAD_DIM, 2 * samples * token_rows), jnp.bfloat16
        ),
        in_specs=[pl.BlockSpec(memory_space=pltpu.SMEM)] * 2 + [vmem] * (len(blocks) + 3),
        out_specs=vmem,
        scratch_shapes=[pltpu.VMEM((len(blocks), pair_rows, width), jnp.bfloat16)],
        compiler_params=pltpu.CompilerParams(vmem_limit_bytes=48 * 1024 * 1024),
        cost_estimate=pl.CostEstimate(
            flops=flops, bytes_accessed=6 * 1024 * 1024, transcendentals=samples * 2 * total * total
        ),
        name="attend",
    )(info_1, info_2, *blocks, w, bias_a, bias_b)


def per_device(
    pair_repr,
    asym_id,
    valid_len,
    rel_embed,
    pair_gain,
    bias_weight,
    tokens,
    token_gain,
    qkv_weight,
    out_weight,
):
    sample_count, _, width = tokens.shape
    total = asym_id.shape[0]
    rows = lax.axis_size("row")
    cols = lax.axis_size("col")
    tile_rows, tile_cols, _ = pair_repr.shape
    pairs = rows // 2
    z = lax.axis_index("row")
    side = z % 2
    col = lax.axis_index("col")
    core = lax.axis_index("samp")
    swap = [(0, 1), (1, 0)]
    def shifted(value, axis, by):
        size = lax.axis_size(axis)
        return lax.ppermute(value, axis, [(i, (i + by) % size) for i in range(size)])

    info_1 = jnp.stack([valid_len[0], side]).astype(jnp.int32)
    info_2 = jnp.stack([core, z // 2, valid_len[0]]).astype(jnp.int32)

    depth = out_weight.shape[1]
    slice_rows, half_width = depth // cols, width // 2
    piece = lax.dynamic_slice(
        out_weight[0], (col * slice_rows, core * half_width), (slice_rows, half_width)
    )

    half_samples = sample_count // 2
    keep, give = normalized_halves(side.reshape(1), tokens, token_gain)
    neighbour = [(i, i ^ 1) for i in range(rows)]
    given = lax.ppermute(give, "row", neighbour)
    up = down = jnp.concatenate([keep, given])
    blocks = [up] + [None] * (pairs - 1)
    for step in range(1, pairs // 2 + 1):
        up = shifted(up, "row", 2)
        if step < pairs // 2:
            down = shifted(down, "row", -2)
            blocks[-step] = down
        blocks[step] = up

    other_w = lax.ppermute(qkv_weight[0], "row", neighbour)
    own_first = side == core
    w_a = jnp.where(own_first, qkv_weight[0], other_w)
    w_b = jnp.where(own_first, other_w, qkv_weight[0])
    w_pair = jnp.stack([w_a, w_b]).transpose(0, 1, 3, 2).reshape(-1, width)

    tile = bias_tile_of(pair_repr, asym_id, rel_embed, pair_gain, bias_weight)
    lanes = 128
    tile = tile.reshape(pairs, 1, -1, lanes)
    tile_lines = tile.shape[2]
    tile = jnp.broadcast_to(tile, (pairs, 2, tile_lines, lanes)).reshape(rows, tile_lines, lanes)
    piece = piece.astype(jnp.float32).reshape(1, -1, lanes)
    piece = jnp.broadcast_to(piece, (rows, *piece.shape[1:]))
    by_row = exchange(jnp.concatenate([tile, piece], 1), "row")
    pieces = by_row[:, tile_lines:].astype(jnp.bfloat16)
    by_key = by_row[:, :tile_lines].reshape(rows, 2, tile_rows, tile_cols).transpose(1, 3, 0, 2)
    by_key = by_key.reshape(2, tile_cols, total)
    fanned = jnp.broadcast_to(by_key[None], (cols, *by_key.shape))
    bias_a = exchange(fanned.reshape(2 * cols, tile_cols, total), ("col", "samp"))
    bias_a = bias_a.reshape(total, total)
    bias_b = lax.ppermute(bias_a, "samp", swap)

    w_half = pieces.reshape(rows * slice_rows, half_width)
    bit, place = cols // 2, 0
    while bit:
        other = lax.ppermute(w_half, "col", [(i, i ^ bit) for i in range(cols)])
        low = (col & bit) == 0
        w_half = jnp.stack(
            [jnp.where(low, w_half, other), jnp.where(low, other, w_half)], axis=place
        )
        bit, place = bit // 2, place + 1
    other = lax.ppermute(w_half, "samp", swap)
    w_out = jnp.concatenate(
        [jnp.where(core == 0, w_half, other), jnp.where(core == 0, other, w_half)], axis=-1
    )
    w_out = w_out.reshape(cols, rows, slice_rows, width).transpose(1, 0, 2, 3)
    w_out = w_out.reshape(width, width)

    attended = attend(info_1, info_2, blocks, w_pair, bias_a, bias_b, half_samples)
    back = exchange(attended, "row")
    return output(back, w_out, tokens)


def solution(mesh):
    return jax.shard_map(
        per_device,
        mesh=mesh,
        in_specs=(
            P(("job", "row"), ("col", "samp"), None),
            P("job"),
            P("job"),
            P(),
            P(),
            P(),
            P(("job", "col", "samp"), "row", None),
            P(),
            P(None, None, None, "row"),
            P(None, "row", None),
        ),
        out_specs=P(("job", "col", "samp"), "row", None),
        check_vma=False,
    )
```

```python
import functools
import math

import jax
import jax.numpy as jnp
from jax import lax
from jax.experimental import pallas as pl
from jax.experimental.pallas import tpu as pltpu
from jax.sharding import PartitionSpec as P


HEAD_DIM = 48

epsilon = 1e-05


def normalize(values, gain_vector):
    average = jnp.mean(values, axis=-1, keepdims=True)
    centered = values - average
    variance = jnp.mean(centered * centered, axis=-1, keepdims=True)
    return centered * lax.rsqrt(variance + epsilon) * gain_vector


def exchange(blocks, axis, groups=None):
    return lax.all_to_all(
        blocks, axis, split_axis=0, concat_axis=0, axis_index_groups=groups, tiled=True
    )


def bias_tile_of(pair_repr, asym_id, rel_embed, pair_gain, bias_weight):
    tile_rows, tile_cols, channels = pair_repr.shape
    bin_count = rel_embed.shape[0]
    reach_max = bin_count // 2 - 1
    first_row = lax.axis_index("row") * tile_rows
    first_col = lax.axis_index(("col", "samp")) * tile_cols
    row_ids = first_row + jnp.arange(tile_rows, dtype=jnp.int32)
    col_ids = first_col + jnp.arange(tile_cols, dtype=jnp.int32)
    row_chain = lax.dynamic_slice_in_dim(asym_id, first_row, tile_rows, 0)
    col_chain = lax.dynamic_slice_in_dim(asym_id, first_col, tile_cols, 0)
    offset = jnp.clip(row_ids[:, None] - col_ids[None, :], -reach_max, reach_max) + reach_max
    bin_ids = jnp.where(row_chain[:, None] == col_chain[None, :], offset, bin_count - 1)
    onehot = (
        bin_ids.reshape(-1)[:, None] == jnp.arange(bin_count, dtype=jnp.int32)[None, :]
    ).astype(jnp.bfloat16)
    summed = pair_repr.reshape(-1, channels).astype(jnp.float32) + jnp.dot(
        onehot, rel_embed, preferred_element_type=jnp.float32
    )
    normed = normalize(summed, pair_gain).astype(jnp.bfloat16)
    projected = lax.dot_general(
        bias_weight, normed, (((0,), (1,)), ((), ())), preferred_element_type=jnp.float32
    )
    return projected


def normalize_kernel(side_ref, tokens_ref, gain_ref, keep_ref, give_ref):
    samples, token_rows, width = tokens_ref.shape
    values = tokens_ref[...].reshape(samples * token_rows, width).astype(jnp.float32)
    normed = normalize(values, gain_ref[...]).astype(jnp.bfloat16)
    half = samples * token_rows // 2
    even = side_ref[0] == 0
    keep_ref[...] = jnp.where(even, normed[:half], normed[half:])
    give_ref[...] = jnp.where(even, normed[half:], normed[:half])


def normalized_halves(side, tokens, gain):
    samples, token_rows, width = tokens.shape
    half = jax.ShapeDtypeStruct((samples * token_rows // 2, width), jnp.bfloat16)
    vmem = pl.BlockSpec(memory_space=pltpu.VMEM)
    return pl.pallas_call(
        normalize_kernel,
        out_shape=(half, half),
        in_specs=[pl.BlockSpec(memory_space=pltpu.SMEM), vmem, vmem],
        out_specs=(vmem, vmem),
        cost_estimate=pl.CostEstimate(
            flops=10 * tokens.size, bytes_accessed=4 * tokens.size, transcendentals=0
        ),
        name="normalize",
    )(side, tokens, gain)


def attend_kernel(info_1_ref, info_2_ref, *refs, samples, scale):
    *block_refs, w_ref, bias_a_ref, bias_b_ref, out_ref, blocks_ref = refs
    pairs, pair_rows, _ = blocks_ref.shape
    half_rows = pair_rows // 2
    token_rows = half_rows // samples
    total = bias_a_ref.shape[0]
    valid, side, core, pair = info_1_ref[0], info_1_ref[1], info_2_ref[0], info_2_ref[1]
    key_ok = lax.broadcasted_iota(jnp.int32, (total, 1), 0) < valid
    dot = functools.partial(lax.dot_general, preferred_element_type=jnp.float32)
    for step, block_ref in enumerate(block_refs):
        blocks_ref[lax.rem(pair - step + pairs, pairs)] = block_ref[...]
    swapped = core == 1
    ordered = [[], []]
    starts = [side * half_rows, (1 - side) * half_rows]
    for u in range(samples):
        x = jnp.concatenate(
            [
                blocks_ref[k, pl.ds(pl.multiple_of(start + u * token_rows, token_rows), token_rows), :]
                for k in range(pairs)
                for start in starts
            ]
        )
        projected = dot(w_ref[...], x, (((1,), (1,)), ((), ()))).astype(jnp.bfloat16)
        outs = []
        for h, bias_ref in enumerate((bias_a_ref, bias_b_ref)):
            query, key, value = (
                projected[(h * 3 + p) * HEAD_DIM : (h * 3 + p + 1) * HEAD_DIM] for p in range(3)
            )
            scores = dot(key, query, (((0,), (0,)), ((), ()))) * scale + bias_ref[...]
            scores = jnp.where(key_ok, scores, -1e30)
            row_max = jnp.max(scores, axis=0, keepdims=True)
            weights = jnp.where(key_ok, jnp.exp(scores - row_max), 0.0)
            inverse = 1.0 / jnp.sum(weights, axis=0, keepdims=True)
            probs = (weights * inverse).astype(jnp.bfloat16)
            outs.append(dot(value, probs, (((1,), (0,)), ((), ()))))
        ordered[0].append(jnp.where(swapped, outs[1], outs[0]))
        ordered[1].append(jnp.where(swapped, outs[0], outs[1]))
    for i in range(total // token_rows):
        at = slice(i * token_rows, (i + 1) * token_rows)
        out_ref[i] = jnp.concatenate(
            [value[:, at] for head in ordered for value in head], axis=1
        ).astype(jnp.bfloat16)


def output_kernel(core_ref, back_ref, own_ref, other_ref, tokens_ref, out_ref):
    rows, _, lanes = back_ref.shape
    half_samples = tokens_ref.shape[0] // 2
    half = lanes // 2
    width = own_ref.shape[1]
    core = core_ref[0]
    for side in range(2):
        pieces = []
        for k in range(rows // 2):
            block = back_ref[2 * k + side].astype(jnp.float32)
            pieces += [block[:, :half], block[:, half:]]
        attended = jnp.concatenate(pieces).astype(jnp.bfloat16)
        samples = pl.ds(side * half_samples, half_samples)
        for w_ref, place in ((own_ref, core), (other_ref, 1 - core)):
            update = lax.dot_general(
                attended, w_ref[...], (((0,), (0,)), ((), ())), preferred_element_type=jnp.float32
            )
            columns = pl.ds(pl.multiple_of(place * width, 128), width)
            before = tokens_ref[samples, :, columns].astype(jnp.float32)
            after = before + update.reshape(before.shape)
            out_ref[samples, :, columns] = after.astype(jnp.bfloat16)


def output(core, back, own, other, tokens):
    vmem = pl.BlockSpec(memory_space=pltpu.VMEM)
    return pl.pallas_call(
        output_kernel,
        out_shape=jax.ShapeDtypeStruct(tokens.shape, jnp.bfloat16),
        in_specs=[pl.BlockSpec(memory_space=pltpu.SMEM)] + [vmem] * 4,
        out_specs=vmem,
        cost_estimate=pl.CostEstimate(
            flops=2 * tokens.size * own.shape[0], bytes_accessed=4 * 1024 * 1024, transcendentals=0
        ),
        name="output",
    )(core, back, own, other, tokens)


def attend(info_1, info_2, blocks, w, bias_a, bias_b, samples):
    pair_rows, width = blocks[0].shape
    total = bias_a.shape[0]
    token_rows = pair_rows // 2 // samples
    vmem = pl.BlockSpec(memory_space=pltpu.VMEM)
    flops = 2 * samples * total * (width * w.shape[0] + 4 * total * HEAD_DIM)
    return pl.pallas_call(
        functools.partial(attend_kernel, samples=samples, scale=1.0 / math.sqrt(HEAD_DIM)),
        out_shape=jax.ShapeDtypeStruct(
            (total // token_rows, HEAD_DIM, 2 * samples * token_rows), jnp.bfloat16
        ),
        in_specs=[pl.BlockSpec(memory_space=pltpu.SMEM)] * 2 + [vmem] * (len(blocks) + 3),
        out_specs=vmem,
        scratch_shapes=[pltpu.VMEM((len(blocks), pair_rows, width), jnp.bfloat16)],
        compiler_params=pltpu.CompilerParams(vmem_limit_bytes=48 * 1024 * 1024),
        cost_estimate=pl.CostEstimate(
            flops=flops, bytes_accessed=6 * 1024 * 1024, transcendentals=samples * 2 * total * total
        ),
        name="attend",
    )(info_1, info_2, *blocks, w, bias_a, bias_b)


def per_device(
    pair_repr,
    asym_id,
    valid_len,
    rel_embed,
    pair_gain,
    bias_weight,
    tokens,
    token_gain,
    qkv_weight,
    out_weight,
):
    sample_count, _, width = tokens.shape
    total = asym_id.shape[0]
    rows = lax.axis_size("row")
    cols = lax.axis_size("col")
    tile_rows, tile_cols, _ = pair_repr.shape
    pairs = rows // 2
    z = lax.axis_index("row")
    side = z % 2
    col = lax.axis_index("col")
    core = lax.axis_index("samp")
    swap = [(0, 1), (1, 0)]

    def shifted(value, axis, by):
        size = lax.axis_size(axis)
        return lax.ppermute(value, axis, [(i, (i + by) % size) for i in range(size)])

    info_1 = jnp.stack([valid_len[0], side]).astype(jnp.int32)
    info_2 = jnp.stack([core, z // 2, valid_len[0]]).astype(jnp.int32)

    depth = out_weight.shape[1]
    slice_rows, half_width = depth // cols, width // 2
    piece = lax.dynamic_slice(
        out_weight[0], (col * slice_rows, core * half_width), (slice_rows, half_width)
    )

    half_samples = sample_count // 2
    keep, give = normalized_halves(side.reshape(1), tokens, token_gain)
    neighbour = [(i, i ^ 1) for i in range(rows)]
    given = lax.ppermute(give, "row", neighbour)
    up = down = jnp.concatenate([keep, given])
    blocks = [up] + [None] * (pairs - 1)
    for step in range(1, pairs // 2 + 1):
        up = shifted(up, "row", 2)
        if step < pairs // 2:
            down = shifted(down, "row", -2)
            blocks[-step] = down
        blocks[step] = up

    other_w = lax.ppermute(qkv_weight[0], "row", neighbour)
    own_first = side == core
    w_a = jnp.where(own_first, qkv_weight[0], other_w)
    w_b = jnp.where(own_first, other_w, qkv_weight[0])
    w_pair = jnp.stack([w_a, w_b]).transpose(0, 1, 3, 2).reshape(-1, width)

    tile = bias_tile_of(pair_repr, asym_id, rel_embed, pair_gain, bias_weight)
    lanes = 128
    tile = tile.reshape(pairs, 1, -1, lanes)
    tile_lines = tile.shape[2]
    tile = jnp.broadcast_to(tile, (pairs, 2, tile_lines, lanes)).reshape(rows, tile_lines, lanes)
    piece = piece.astype(jnp.float32).reshape(1, -1, lanes)
    piece = jnp.broadcast_to(piece, (rows, *piece.shape[1:]))
    by_row = exchange(jnp.concatenate([tile, piece], 1), "row")
    pieces = by_row[:, tile_lines:].astype(jnp.bfloat16)
    by_key = by_row[:, :tile_lines].reshape(rows, 2, tile_rows, tile_cols).transpose(1, 3, 0, 2)
    by_key = by_key.reshape(2, tile_cols, total)
    fanned = jnp.broadcast_to(by_key[None], (cols, *by_key.shape))
    bias_a = exchange(fanned.reshape(2 * cols, tile_cols, total), ("col", "samp"))
    bias_a = bias_a.reshape(total, total)
    bias_b = lax.ppermute(bias_a, "samp", swap)

    w_half = pieces.reshape(rows * slice_rows, half_width)
    bit, place = cols // 2, 0
    while bit:
        other = lax.ppermute(w_half, "col", [(i, i ^ bit) for i in range(cols)])
        low = (col & bit) == 0
        w_half = jnp.stack(
            [jnp.where(low, w_half, other), jnp.where(low, other, w_half)], axis=place
        )
        bit, place = bit // 2, place + 1
    other = lax.ppermute(w_half, "samp", swap)

    def arranged(half):
        half = half.reshape(cols, rows, slice_rows, half_width).transpose(1, 0, 2, 3)
        return half.reshape(width, half_width)

    attended = attend(info_1, info_2, blocks, w_pair, bias_a, bias_b, half_samples)
    back = exchange(attended, "row")
    return output(core.reshape(1), back, arranged(w_half), arranged(other), tokens)


def solution(mesh):
    return jax.shard_map(
        per_device,
        mesh=mesh,
        in_specs=(
            P(("job", "row"), ("col", "samp"), None),
            P("job"),
            P("job"),
            P(),
            P(),
            P(),
            P(("job", "col", "samp"), "row", None),
            P(),
            P(None, None, None, "row"),
            P(None, "row", None),
        ),
        out_specs=P(("job", "col", "samp"), "row", None),
        check_vma=False,
    )
```
